128 devices in a mesh: gx: 4 (over y), gy: 4 (over z), gz: 8 (over x, core).
Axes of the slice: x: 4, y: 4, z: 4, core: 2. Of those that a mesh axis runs over, the one named last changes fastest.
Arguments:
- tokens: bfloat16 [1024, 7168], P(('gx', 'gy', 'gz')), may hold values from -6 to 6
- expert_ids: int32 [1024, 8], P(('gx', 'gy', 'gz')), may hold values from 0 to 15, as said below
- slot_ids: int32 [1024, 8], P(('gx', 'gy', 'gz')), may hold values from 0 to 7, as said below
- route_weight: bfloat16 [1024, 8], P(('gx', 'gy', 'gz')), may hold values from 0.099609375 to 0.59765625
- gate_weight: bfloat16 [16, 7168, 2048], P(('gx', 'gy'), None, 'gz'), may hold values from -0.0625 to 0.0625
- up_weight: bfloat16 [16, 7168, 2048], P(('gx', 'gy'), None, 'gz'), may hold values from -0.0625 to 0.0625
- down_weight: bfloat16 [16, 2048, 7168], P(('gx', 'gy'), 'gz'), may hold values from -0.125 to 0.125
- expert_bias: float32 [16], replicated, may hold values from -3 to 3
Outputs:
- combined: bfloat16 [1024, 7168], P(('gx', 'gy', 'gz'))
- expert_load: int32 [16], replicated
- new_bias: float32 [16], replicated
The draws below stay inside these ranges and needn't reach their ends.
Inputs may be any that keep to these rules, and one draw needn't show every extreme that they name: `expert_ids`: the 8 experts of a token are different. Among the 8 tokens of one device no expert is named more than 8 times; one expert is named by every token of every device. `slot_ids`: for each device and expert, the routes of that device's tokens to that expert hold different slots.
All inputs are finite; a program needn't handle non-finite values.
Results may differ from the reference program's by a relative error of at most 0.015.
Values may be sent and summed in bfloat16 or wider, within the bound.
No kernel may reach another device: no remote copies, remote signals or barrier semaphores. Data moves between devices by JAX's collectives and lax.ppermute only.
A program may use at most 128 MiB of HBM per device.

```python
import jax
import jax.numpy as jnp
from jax import lax

D = 7168
FF = 2048
TOPK = 8
TOK_DEV = 8
PLACE_LIMIT = 8
HID_PARTS = 8
FF_PART = 256
EXPERTS = 16
TOKENS = 1024


def route_tables(key):
    base = jax.random.fold_in(key, 31)
    keys = jax.random.split(base, 5)
    blocks = TOKENS // TOK_DEV
    expert_index = jnp.arange(EXPERTS, dtype=jnp.int32)
    roots = jax.random.randint(keys[0], (EXPERTS,), 0, 64)
    favorite = jax.random.randint(keys[1], (), 0, EXPERTS)
    overfull_mask = roots * roots + 100000 * (expert_index == favorite).astype(jnp.int32)
    block_index = jnp.arange(blocks, dtype=jnp.int32)
    window_start = block_index * EXPERTS // blocks
    within_window = (expert_index[None, :] - window_start[:, None]) % EXPERTS < EXPERTS // 2
    window_reward = 4000 * within_window.astype(jnp.int32)
    random_noise = jax.random.randint(keys[2], (blocks, TOK_DEV, EXPERTS), 0, 2000)
    cyclic_offset = jax.random.randint(keys[3], (blocks, TOK_DEV), 0, EXPERTS)
    shuffle = jax.random.randint(keys[4], (blocks, EXPERTS, PLACE_LIMIT), 0, 1 << 20) * PLACE_LIMIT + jnp.arange(PLACE_LIMIT, dtype=jnp.int32)
    rankings = jnp.argsort(shuffle, axis=-1, stable=True).astype(jnp.int32)

    def lone_portion(jitter_entries, shifted_entries, preference_order, interval_extra_vector):

        def advance(places_filled, inputs):
            present_jitter, rotation_now = inputs
            gating_scores = jnp.where(places_filled >= PLACE_LIMIT, -1, overfull_mask + interval_extra_vector + present_jitter)
            keyed = gating_scores * EXPERTS + (expert_index + rotation_now) % EXPERTS
            _, chosen = lax.top_k(keyed, TOPK)
            chosen = chosen.astype(jnp.int32)
            arrival = places_filled[chosen]
            slot_now = preference_order[chosen, arrival]
            hits_now = jnp.sum((chosen[:, None] == expert_index[None, :]).astype(jnp.int32), axis=0)
            return (places_filled + hits_now, (chosen, slot_now))
        _, (selected_experts, slot_buffer) = lax.scan(advance, jnp.zeros((EXPERTS,), jnp.int32), (jitter_entries, shifted_entries))
        return (selected_experts, slot_buffer)
    selected_experts, slot_buffer = jax.vmap(lone_portion)(random_noise, cyclic_offset, rankings, window_reward)
    return (selected_experts.reshape(TOKENS, TOPK).astype(jnp.int32), slot_buffer.reshape(TOKENS, TOPK).astype(jnp.int32))


def draw_expert_ids(key, part):
    return route_tables(key)[0]


def draw_slot_ids(key, part):
    return route_tables(key)[1]


def block_levels(key, extent, cuts, low, largest):
    def one(dim, parts):
        steps = jax.random.uniform(jax.random.fold_in(jax.random.fold_in(key, 6), dim), (parts,), jnp.float32, low / len(cuts), largest / len(cuts))
        return jnp.repeat(jnp.exp(steps), extent[dim] // parts).reshape((-1,) + (1,) * (len(extent) - dim - 1))

    factor_of = one(*cuts[0])
    for cut in cuts[1:]:
        factor_of = factor_of * one(*cut)
    return factor_of


def normal_values(rng, shape, spread, reach, cuts=(), kind=jnp.bfloat16):
    loudness = block_levels(rng, shape, cuts, -0.22, 0.18) if cuts else 1.0
    result = jax.random.normal(rng, shape, jnp.float32) * spread * loudness
    return jnp.minimum(jnp.maximum(result, -reach), reach).astype(kind)


def setup_inputs(seed: int = 0) -> dict:
    streams_of = jax.random.split(jax.random.key(seed), 9)
    tokens = normal_values(streams_of[0], (TOKENS, D), 1.0, 6.0, ((0, 128),))
    expert_ids = draw_expert_ids(jax.random.fold_in(streams_of[8], 71), 0)
    slot_ids = draw_slot_ids(jax.random.fold_in(streams_of[8], 71), 0)
    route_weight = jnp.clip(0.099609375 + 0.49804688 * jax.random.uniform(streams_of[3], (TOKENS, TOPK), jnp.float32) ** block_levels(streams_of[3], (TOKENS, TOPK), ((0, 128),), -0.2, 0.2), 0.099609375, 0.59765625).astype(jnp.bfloat16)
    gate_weight = normal_values(streams_of[4], (EXPERTS, D, FF), D ** -0.5, 0.0625, ((0, 16), (2, 8)))
    up_weight = normal_values(streams_of[5], (EXPERTS, D, FF), D ** -0.5, 0.0625, ((0, 16), (2, 8)))
    down_weight = normal_values(streams_of[6], (EXPERTS, FF, D), FF ** -0.5, 0.125, ((0, 16), (1, 8)))
    expert_bias = normal_values(streams_of[7], (EXPERTS,), 0.5, 3.0, (), jnp.float32)
    return dict(tokens=tokens, expert_ids=expert_ids, slot_ids=slot_ids, route_weight=route_weight, gate_weight=gate_weight, up_weight=up_weight, down_weight=down_weight, expert_bias=expert_bias)


bias_rate = 0.001


def reference(tokens, expert_ids, slot_ids, route_weight, gate_weight, up_weight, down_weight, expert_bias):
    sources = TOKENS // TOK_DEV
    source = jnp.broadcast_to((jnp.arange(TOKENS, dtype=jnp.int32) // TOK_DEV)[:, None], (TOKENS, TOPK))
    buffer = jnp.zeros((EXPERTS, sources, PLACE_LIMIT, D), jnp.bfloat16)
    buffer = buffer.at[expert_ids, source, slot_ids].set(jnp.broadcast_to(tokens[:, None, :], (TOKENS, TOPK, D)))

    def run_expert(inputs):
        rows_in, gate_mat, up_mat, down_mat = inputs
        flat_rows = rows_in.reshape(sources * PLACE_LIMIT, D)
        gate_act = jnp.dot(flat_rows, gate_mat, preferred_element_type=jnp.float32)
        up_act = jnp.dot(flat_rows, up_mat, preferred_element_type=jnp.float32)
        hidden = (jax.nn.silu(gate_act) * up_act).astype(jnp.bfloat16)
        total = jnp.zeros((sources * PLACE_LIMIT, D), jnp.float32)
        for segment in range(HID_PARTS):
            begin_at = segment * FF_PART
            partial_out = jnp.dot(hidden[:, begin_at:begin_at + FF_PART], down_mat[begin_at:begin_at + FF_PART], preferred_element_type=jnp.float32).astype(jnp.bfloat16)
            total = total + lax.optimization_barrier(partial_out).astype(jnp.float32)
        return total.astype(jnp.bfloat16).reshape(sources, PLACE_LIMIT, D)

    results = lax.map(run_expert, (buffer, gate_weight, up_weight, down_weight))
    selected_experts = results[expert_ids, source, slot_ids]
    combined = jnp.sum(route_weight.astype(jnp.float32)[:, :, None] * selected_experts.astype(jnp.float32), axis=1).astype(jnp.bfloat16)
    counts = jnp.sum((expert_ids[:, :, None] == jnp.arange(EXPERTS, dtype=jnp.int32)).astype(jnp.int32), axis=(0, 1))
    mean_load = TOKENS * TOPK // EXPERTS
    new_bias = expert_bias + bias_rate * jnp.sign((mean_load - counts).astype(jnp.float32))
    return (combined, counts, new_bias)
```

```python
import jax
import jax.numpy as jnp
from jax import lax
from jax.sharding import Mesh
from jax.sharding import PartitionSpec as P

AXES = ("gx", "gy", "gz_0", "gz_1")
GZ = ("gz_0", "gz_1")
X, Y, Z = "gz_0", "gx", "gy"
EARLY = (X, Y, Z)
LATE = ((X, Y, Z), (Y, Z, X), (Z, X, Y))
INFO = 128
BF16 = jnp.bfloat16
F32 = jnp.float32

bias_rate = 0.001


def exchange(value, axis, step):
    masks = (1, 3) if step == 0 else (3, 1)
    pairs = [(2 * i + c, 2 * (i ^ masks[c]) + c) for i in range(4) for c in range(2)]
    return lax.ppermute(value, (axis, "gz_1"), pairs)


def partner(value):
    return lax.ppermute(value, "gz_1", [(0, 1), (1, 0)])


def reorder(rows, source, target):
    blocks = rows.reshape((2, 2, 2, rows.shape[0] // 8) + rows.shape[1:])
    order = [2 - source.index(target[2 - i]) for i in range(3)]
    return blocks.transpose(order + list(range(3, blocks.ndim))).reshape(rows.shape)


def body(
    tokens, expert_ids, slot_ids, route_weight, gate_weight, up_weight, down_weight, expert_bias
):
    experts = lax.axis_size("gx") * lax.axis_size("gy")
    devices = experts * lax.axis_size(GZ)
    tok_rows, width = tokens.shape
    route_count = expert_ids.shape[1]
    own_expert = lax.axis_index("gx") * lax.axis_size("gy") + lax.axis_index("gy")

    gate_own, up_own, down_own = gate_weight[0], up_weight[0], down_weight[0]
    gate_far, up_far, down_far = partner(gate_own), partner(up_own), partner(down_own)
    gate_ups = (gate_own, gate_far, up_own, up_far)

    named = expert_ids[:, :, None] == jnp.arange(experts, dtype=jnp.int32)
    weight_of = jnp.sum(jnp.where(named, route_weight.astype(F32)[:, :, None], 0.0), axis=1)
    marks = jnp.sum(named.astype(F32), axis=1)
    info = jnp.concatenate([weight_of, marks], axis=1)
    info = jnp.pad(info, ((0, 0), (0, INFO - 2 * experts))).astype(BF16)

    rows = jnp.concatenate([tokens, info], axis=1)
    for axis in EARLY:
        rows = jnp.concatenate([rows, exchange(rows, axis, 0)], axis=0)
    cuts = (0, 2560, 4864, width + INFO)
    pieces = [rows[:, cuts[i] : cuts[i + 1]] for i in range(3)]
    for step in range(2):
        pieces = [
            jnp.concatenate([p, exchange(p, LATE[i][step], 1)], axis=0)
            for i, p in enumerate(pieces)
        ]
    far_pieces = [exchange(p, LATE[i][2], 1) for i, p in enumerate(pieces)]

    acts = [None] * 4
    for i in range(3):
        top = min(cuts[i + 1], width)
        for j, w in enumerate(gate_ups):
            w_cut = lax.slice_in_dim(w, cuts[i], top, axis=0)
            both = jnp.concatenate(
                [
                    jnp.dot(p[:, : top - cuts[i]], w_cut, preferred_element_type=F32)
                    for p in (pieces[i], far_pieces[i])
                ],
                axis=0,
            )
            both = reorder(both, LATE[i], LATE[0])
            acts[j] = both if acts[j] is None else acts[j] + both
    route_rows = jnp.concatenate(
        [pieces[2][:, width - cuts[2] :], far_pieces[2][:, width - cuts[2] :]], axis=0
    )
    route_rows = reorder(route_rows, LATE[2], LATE[0]).astype(F32)
    mine = (jnp.arange(INFO, dtype=jnp.int32) == own_expert).astype(F32)
    row_weight = jnp.sum(route_rows * mine, axis=1, keepdims=True)
    hidden = jnp.concatenate(
        [(jax.nn.silu(acts[j]) * acts[j + 2] * row_weight).astype(BF16) for j in range(2)], axis=1
    )

    half_load = jnp.sum(route_rows, axis=0)[experts : 2 * experts].astype(jnp.int32)
    expert_load = half_load + partner(half_load)
    mean_load = tok_rows * devices * route_count // experts
    new_bias = expert_bias + bias_rate * jnp.sign((mean_load - expert_load).astype(F32))

    down = jnp.concatenate([down_own, down_far], axis=0)
    col_cuts = (0, 2432, 4864, width)
    kept, sent = [], []
    for i in range(3):
        h = reorder(hidden, LATE[0], LATE[i])
        d = down[:, col_cuts[i] : col_cuts[i + 1]]
        half = h.shape[0] // 2
        sent.append(jnp.dot(h[half:], d, preferred_element_type=F32).astype(BF16))
        kept.append(jnp.dot(h[:half], d, preferred_element_type=F32))
    for step in (2, 1, 0):
        got = [exchange(sent[i], LATE[i][step], 1) for i in range(3)]
        totals = [kept[i] + got[i].astype(F32) for i in range(3)]
        half = totals[0].shape[0] // 2
        if step:
            sent = [t[half:].astype(BF16) for t in totals]
            kept = [t[:half] for t in totals]
    total = jnp.concatenate(totals, axis=1)
    for axis in reversed(EARLY):
        half = total.shape[0] // 2
        got = exchange(total[half:].astype(BF16), axis, 0)
        total = total[:half] + got.astype(F32)
    return (total.astype(BF16), expert_load, new_bias)


def solution(mesh):
    finer = Mesh(mesh.devices.reshape(mesh.shape["gx"], mesh.shape["gy"], 4, 2), AXES)
    return jax.shard_map(
        body,
        mesh=finer,
        in_specs=(
            P(AXES, None),
            P(AXES, None),
            P(AXES, None),
            P(AXES, None),
            P(("gx", "gy"), None, GZ),
            P(("gx", "gy"), None, GZ),
            P(("gx", "gy"), GZ, None),
            P(),
        ),
        out_specs=(P(AXES, None), P(), P()),
        check_vma=False,
    )
```

```python
import functools

import jax
import jax.numpy as jnp
from jax import lax
from jax.experimental import pallas as pl
from jax.experimental.pallas import tpu as pltpu
from jax.sharding import Mesh
from jax.sharding import PartitionSpec as P

AXES = ("gx", "gy", "gz_0", "gz_1")
GZ = ("gz_0", "gz_1")
X, Y, Z = "gz_0", "gx", "gy"
EARLY = (X, Y, Z)
LATE = ((X, Y, Z), (Y, Z, X), (Z, X, Y))
INFO = 128
CUTS = (0, 2560, 4864, 7168)
COL_CUTS = (0, 2432, 4864, 7168)
BF16 = jnp.bfloat16
F32 = jnp.float32

bias_rate = 0.001


def exchange(value, axis):
    masks = (3, 1)
    pairs = [(2 * i + c, 2 * (i ^ masks[c]) + c) for i in range(4) for c in range(2)]
    return lax.ppermute(value, (axis, "gz_1"), pairs)


def direct(value, hops):
    masks = (1, 3)
    pairs = []
    for a in range(4):
        for b in range(4):
            for x in range(4):
                for c in range(2):
                    m = masks[c]
                    far = (
                        a ^ (m if Y in hops else 0),
                        b ^ (m if Z in hops else 0),
                        x ^ (m if X in hops else 0),
                    )
                    here = ((a * 4 + b) * 4 + x) * 2 + c
                    pairs.append((here, ((far[0] * 4 + far[1]) * 4 + far[2]) * 2 + c))
    return lax.ppermute(value, AXES, pairs)


def hops_of(n):
    return [axis for k, axis in enumerate(EARLY) if n >> k & 1]


def partner(value):
    return lax.ppermute(value, "gz_1", [(0, 1), (1, 0)])


def canonical(colour, place):
    bits = {LATE[colour][k]: place >> k & 1 for k in range(3)}
    return sum(bits[LATE[0][k]] << k for k in range(3))


def gate_up_kernel(finish, *refs):
    if finish:
        expert, x0, x1, x2, w0, w1, w2, w3, near_x2, acc_in, hidden, *scratch = refs
    else:
        x0, x1, x2, w0, w1, w2, w3, out, *scratch = refs
    xs, ws = (x0, x1, x2), (w0, w1, w2, w3)
    b0, b1, b2, wbuf, xsem, wsem = scratch[:6]
    bufs = (b0, b1, b2)
    acc = scratch[6] if finish else out
    copies_x = [pltpu.make_async_copy(xs[i], bufs[i], xsem.at[i]) for i in range(3)]
    copies_w = [
        [
            pltpu.make_async_copy(
                ws[j].at[pl.ds(CUTS[i], CUTS[i + 1] - CUTS[i]), :],
                wbuf.at[j, pl.ds(CUTS[i], CUTS[i + 1] - CUTS[i]), :],
                wsem.at[i, j],
            )
            for j in range(4)
        ]
        for i in range(3)
    ]
    for i in range(3):
        copies_x[i].start()
        for j in range(4):
            copies_w[i][j].start()
        if finish and i == 0:
            acc_copy = pltpu.make_async_copy(acc_in, acc, scratch[8].at[0])
            acc_copy.start()
    if finish:
        info = scratch[7]
        near_info = pltpu.make_async_copy(
            near_x2.at[:, pl.ds(CUTS[3] - CUTS[2], INFO)], info, scratch[8].at[1]
        )
        near_info.start()
        acc_copy.wait()
    for i in range(3):
        copies_x[i].wait()
        width = CUTS[i + 1] - CUTS[i]
        for j in range(4):
            copies_w[i][j].wait()
            part = jnp.dot(
                bufs[i][:, :width],
                wbuf[j, CUTS[i] : CUTS[i + 1], :],
                preferred_element_type=F32,
            )
            places = [canonical(i, q + (4 if finish else 0)) for q in range(4)]
            for q, s in enumerate(places):
                rows = part[64 * q : 64 * q + 64]
                if not finish and i == 0:
                    acc[j, 64 * s : 64 * s + 64, :] = rows
                else:
                    acc[j, 64 * s : 64 * s + 64, :] += rows
            if not finish and i == 0:
                for s in range(8):
                    if s not in places:
                        acc[j, 64 * s : 64 * s + 64, :] = jnp.zeros((64, 256), F32)
    if not finish:
        return
    near_info.wait()
    lane = lax.broadcasted_iota(jnp.int32, (64, INFO), 1)
    for place in range(8):
        s = canonical(2, place)
        if place < 4:
            marks = info[64 * place : 64 * place + 64, :]
        else:
            marks = b2[64 * place - 256 : 64 * place - 192, CUTS[3] - CUTS[2] :]
        picked = jnp.where(lane == expert[0], marks.astype(F32), 0.0)
        scale = jnp.sum(picked, axis=1, keepdims=True)
        for part in range(2):
            g = acc[part, 64 * s : 64 * s + 64, :]
            u = acc[part + 2, 64 * s : 64 * s + 64, :]
            h = g / (1.0 + jnp.exp(-g)) * u * scale
            hidden[64 * s : 64 * s + 64, 256 * part : 256 * part + 256] = h.astype(BF16)


def gate_up(pieces, weights, extra=None):
    finish = extra is not None
    hbm = pl.BlockSpec(memory_space=pl.ANY)
    vmem = pl.BlockSpec(memory_space=pltpu.VMEM)
    scratch = [pltpu.VMEM(p.shape, BF16) for p in pieces]
    scratch += [
        pltpu.VMEM((4, CUTS[3], 256), BF16),
        pltpu.SemaphoreType.DMA((3,)),
        pltpu.SemaphoreType.DMA((3, 4)),
    ]
    if finish:
        expert, near_x2, acc = extra
        scratch += [
            pltpu.VMEM((4, 512, 256), F32),
            pltpu.VMEM((256, INFO), BF16),
            pltpu.SemaphoreType.DMA((2,)),
        ]
        args = (expert, *pieces, *weights, near_x2, acc)
        in_specs = [pl.BlockSpec(memory_space=pltpu.SMEM)] + [hbm] * 9
        out = jax.ShapeDtypeStruct((512, 512), BF16)
    else:
        args = (*pieces, *weights)
        in_specs = [hbm] * 7
        out = jax.ShapeDtypeStruct((4, 512, 256), F32)
    return pl.pallas_call(
        functools.partial(gate_up_kernel, finish),
        out_shape=out,
        in_specs=in_specs,
        out_specs=vmem,
        scratch_shapes=scratch,
        compiler_params=pltpu.CompilerParams(vmem_limit_bytes=32 << 20),
        cost_estimate=pl.CostEstimate(
            flops=2 * 256 * 7168 * 1024, transcendentals=0, bytes_accessed=18 << 20
        ),
        name="gate_up_far" if finish else "gate_up_near",
    )(*args)


def down_kernel(colour, far, chunks, hidden, own, other, out, buf, sem):
    start = COL_CUTS[colour]
    copies, at = [], 0
    for n, size in enumerate(chunks):
        for k, w in enumerate((own, other)):
            copies.append(
                pltpu.make_async_copy(
                    w.at[:, pl.ds(start + at, size)],
                    buf.at[pl.ds(256 * k, 256), pl.ds(at, size)],
                    sem.at[n, k],
                )
            )
        at += size
    for c in copies:
        c.start()
    blocks = [canonical(colour, q + (4 if far else 0)) for q in range(4)]
    lhs = jnp.concatenate([hidden[64 * s : 64 * s + 64, :] for s in blocks], axis=0)
    at = 0
    for n, size in enumerate(chunks):
        copies[2 * n].wait()
        copies[2 * n + 1].wait()
        part = jnp.dot(lhs, buf[:, at : at + size], preferred_element_type=F32)
        out[:, at : at + size] = part.astype(out.dtype)
        at += size


def down_part(colour, far, hidden, own, other):
    width = COL_CUTS[colour + 1] - COL_CUTS[colour]
    chunks = (512, 640, 640, 640) if width == 2432 else (768, 768, 768)
    hbm = pl.BlockSpec(memory_space=pl.ANY)
    vmem = pl.BlockSpec(memory_space=pltpu.VMEM)
    return pl.pallas_call(
        functools.partial(down_kernel, colour, far, chunks),
        out_shape=jax.ShapeDtypeStruct((256, width), BF16 if far else F32),
        in_specs=[vmem, hbm, hbm],
        out_specs=vmem,
        scratch_shapes=[
            pltpu.VMEM((512, width), BF16),
            pltpu.SemaphoreType.DMA((len(chunks), 2)),
        ],
        compiler_params=pltpu.CompilerParams(vmem_limit_bytes=16 << 20),
        cost_estimate=pl.CostEstimate(
            flops=2 * 256 * 512 * width, transcendentals=0, bytes_accessed=4 << 20
        ),
        name=f"down_{'far' if far else 'near'}_{colour}",
    )(hidden, own, other)


def body(
    tokens, expert_ids, slot_ids, route_weight, gate_weight, up_weight, down_weight, expert_bias
):
    experts = lax.axis_size("gx") * lax.axis_size("gy")
    devices = experts * lax.axis_size(GZ)
    tok_rows, width = tokens.shape
    route_count = expert_ids.shape[1]
    own_expert = lax.axis_index("gx") * lax.axis_size("gy") + lax.axis_index("gy")

    gate_own, up_own, down_own = gate_weight[0], up_weight[0], down_weight[0]
    gate_far, up_far, down_far = partner(gate_own), partner(up_own), partner(down_own)
    gate_ups = (gate_own, gate_far, up_own, up_far)

    named = expert_ids[:, :, None] == jnp.arange(experts, dtype=jnp.int32)
    weight_of = jnp.sum(jnp.where(named, route_weight.astype(F32)[:, :, None], 0.0), axis=1)
    marks = jnp.sum(named.astype(F32), axis=1)
    info = jnp.concatenate([weight_of, marks], axis=1)
    info = jnp.pad(info, ((0, 0), (0, INFO - 2 * experts))).astype(BF16)

    rows = jnp.concatenate([tokens, info], axis=1)
    rows = jnp.concatenate([rows] + [direct(rows, hops_of(n)) for n in range(1, 8)], axis=0)
    ends = (*CUTS[:3], width + INFO)
    pieces = [rows[:, ends[i] : ends[i + 1]] for i in range(3)]
    for step in range(2):
        pieces = [
            jnp.concatenate([p, exchange(p, LATE[i][step])], axis=0) for i, p in enumerate(pieces)
        ]
    far_pieces = [exchange(p, LATE[i][2]) for i, p in enumerate(pieces)]

    acc = gate_up(pieces, gate_ups)
    expert = jnp.full((1,), own_expert, jnp.int32)
    hidden = gate_up(far_pieces, gate_ups, (expert, pieces[2], acc))

    sent = [down_part(i, True, hidden, down_own, down_far) for i in range(3)]
    kept = [down_part(i, False, hidden, down_own, down_far) for i in range(3)]
    for step in (2, 1, 0):
        got = [exchange(sent[i], LATE[i][step]) for i in range(3)]
        totals = [kept[i] + got[i].astype(F32) for i in range(3)]
        half = totals[0].shape[0] // 2
        if step:
            sent = [t[half:].astype(BF16) for t in totals]
            kept = [t[:half] for t in totals]
    total = jnp.concatenate(totals, axis=1)
    combined = total[:tok_rows]
    for n in range(1, 8):
        block = total[n * tok_rows : (n + 1) * tok_rows].astype(BF16)
        combined = combined + direct(block, hops_of(n)).astype(F32)

    marked = jnp.concatenate([p[:, width - CUTS[2] :] for p in (pieces[2], far_pieces[2])], axis=0)
    half_load = jnp.sum(marked.astype(F32), axis=0)[experts : 2 * experts].astype(jnp.int32)
    expert_load = half_load + partner(half_load)
    mean_load = tok_rows * devices * route_count // experts
    new_bias = expert_bias + bias_rate * jnp.sign((mean_load - expert_load).astype(F32))
    return (combined.astype(BF16), expert_load, new_bias)


def solution(mesh):
    finer = Mesh(mesh.devices.reshape(mesh.shape["gx"], mesh.shape["gy"], 4, 2), AXES)
    return jax.shard_map(
        body,
        mesh=finer,
        in_specs=(
            P(AXES, None),
            P(AXES, None),
            P(AXES, None),
            P(AXES, None),
            P(("gx", "gy"), None, GZ),
            P(("gx", "gy"), None, GZ),
            P(("gx", "gy"), GZ, None),
            P(),
        ),
        out_specs=(P(AXES, None), P(), P()),
        check_vma=False,
    )
```

```python
import functools

import jax
import jax.numpy as jnp
from jax import lax
from jax.experimental import pallas as pl
from jax.experimental.pallas import tpu as pltpu
from jax.sharding import Mesh
from jax.sharding import PartitionSpec as P

AXES = ("gx", "gy", "gz_0", "gz_1")
GZ = ("gz_0", "gz_1")
X, Y, Z = "gz_0", "gx", "gy"
EARLY = (X, Y, Z)
LATE = ((X, Y, Z), (Y, Z, X), (Z, X, Y))
INFO = 128
CUTS = (0, 2560, 4864, 7168)
COL_CUTS = (0, 2432, 4864, 7168)
BF16 = jnp.bfloat16
F32 = jnp.float32

bias_rate = 0.001


def exchange(value, axis):
    masks = (3, 1)
    pairs = [(2 * i + c, 2 * (i ^ masks[c]) + c) for i in range(4) for c in range(2)]
    return lax.ppermute(value, (axis, "gz_1"), pairs)


def direct(value, hops):
    masks = (1, 3)
    pairs = []
    for a in range(4):
        for b in range(4):
            for x in range(4):
                for c in range(2):
                    m = masks[c]
                    far = (
                        a ^ (m if Y in hops else 0),
                        b ^ (m if Z in hops else 0),
                        x ^ (m if X in hops else 0),
                    )
                    here = ((a * 4 + b) * 4 + x) * 2 + c
                    pairs.append((here, ((far[0] * 4 + far[1]) * 4 + far[2]) * 2 + c))
    return lax.ppermute(value, AXES, pairs)


def hops_of(n):
    return [axis for k, axis in enumerate(EARLY) if n >> k & 1]


def partner(value):
    return lax.ppermute(value, "gz_1", [(0, 1), (1, 0)])


def canonical(colour, place):
    bits = {LATE[colour][k]: place >> k & 1 for k in range(3)}
    return sum(bits[LATE[0][k]] << k for k in range(3))


VMEM = pl.BlockSpec(memory_space=pltpu.VMEM)
SMEM = pl.BlockSpec(memory_space=pltpu.SMEM)


def rows_kernel(experts, tokens, ids, weights, out):
    width = tokens.shape[1]
    out[:, :width] = tokens[...]
    lane = lax.broadcasted_iota(jnp.int32, (tokens.shape[0], INFO), 1)
    info = jnp.zeros((tokens.shape[0], INFO), F32)
    for k in range(ids.shape[1]):
        chosen = ids[:, k : k + 1]
        info += jnp.where(lane == chosen, weights[:, k : k + 1].astype(F32), 0.0)
        info += jnp.where(lane == chosen + experts, 1.0, 0.0)
    out[:, width:] = info.astype(BF16)


def rows_of(tokens, ids, weights, experts):
    rows, width = tokens.shape
    return pl.pallas_call(
        functools.partial(rows_kernel, experts),
        out_shape=jax.ShapeDtypeStruct((rows, width + INFO), BF16),
        in_specs=[VMEM] * 3,
        out_specs=VMEM,
        compiler_params=pltpu.CompilerParams(vmem_limit_bytes=4 << 20),
        name="token_rows",
    )(tokens, ids, weights)


def near_kernel(x0, x1, x2, w0, w1, w2, w3, acc):
    for i, x in enumerate((x0, x1, x2)):
        width = CUTS[i + 1] - CUTS[i]
        places = [canonical(i, q) for q in range(4)]
        for j, w in enumerate((w0, w1, w2, w3)):
            part = jnp.dot(
                x[:, :width], w[CUTS[i] : CUTS[i + 1], :], preferred_element_type=F32
            )
            for q, s in enumerate(places):
                rows = part[64 * q : 64 * q + 64]
                if i == 0:
                    acc[j, 64 * s : 64 * s + 64, :] = rows
                else:
                    acc[j, 64 * s : 64 * s + 64, :] += rows
            if i == 0:
                for s in range(8):
                    if s not in places:
                        acc[j, 64 * s : 64 * s + 64, :] = jnp.zeros((64, 256), F32)


def far_kernel(expert, x0, x1, x2, w0, w1, w2, w3, near_x2, acc_in, hidden, marks, acc):
    ready = {}
    for i, x in enumerate((x0, x1, x2)):
        width = CUTS[i + 1] - CUTS[i]
        places = [canonical(i, q + 4) for q in range(4)]
        for j, w in enumerate((w0, w1, w2, w3)):
            part = jnp.dot(
                x[:, :width], w[CUTS[i] : CUTS[i + 1], :], preferred_element_type=F32
            )
            for q, s in enumerate(places):
                rows = part[64 * q : 64 * q + 64]
                before = acc if (j, s) in ready else acc_in
                acc[j, 64 * s : 64 * s + 64, :] = before[j, 64 * s : 64 * s + 64, :] + rows
                ready[j, s] = True
    lane = lax.broadcasted_iota(jnp.int32, (64, INFO), 1)
    sums = jnp.zeros((8, INFO), F32)
    for place in range(8):
        s = canonical(2, place)
        source = near_x2 if place < 4 else x2
        at = 64 * (place % 4)
        info = source[at : at + 64, CUTS[3] - CUTS[2] :].astype(F32)
        sums += jnp.sum(info.reshape(8, 8, INFO), axis=0)
        scale = jnp.sum(jnp.where(lane == expert[0], info, 0.0), axis=1, keepdims=True)
        for part in range(2):
            value = acc if (part, s) in ready else acc_in
            g = value[part, 64 * s : 64 * s + 64, :]
            u = value[part + 2, 64 * s : 64 * s + 64, :]
            h = g / (1.0 + jnp.exp(-g)) * u * scale
            hidden[64 * s : 64 * s + 64, 256 * part : 256 * part + 256] = h.astype(BF16)
    marks[...] = sums


def load_kernel(*refs):
    count = (len(refs) - 1) // 2
    sem = refs[-1]
    copies = [
        pltpu.make_async_copy(refs[k], refs[count + k], sem.at[k]) for k in range(count)
    ]
    for c in copies:
        c.start()
    for c in copies:
        c.wait()


def in_vmem(*arrays):
    return pl.pallas_call(
        load_kernel,
        out_shape=tuple(jax.ShapeDtypeStruct(a.shape, a.dtype) for a in arrays),
        in_specs=[pl.BlockSpec(memory_space=pl.ANY)] * len(arrays),
        out_specs=(VMEM,) * len(arrays),
        scratch_shapes=[pltpu.SemaphoreType.DMA((len(arrays),))],
        compiler_params=pltpu.CompilerParams(vmem_limit_bytes=4 << 20),
        cost_estimate=pl.CostEstimate(flops=8 << 30, transcendentals=0, bytes_accessed=0),
        name="weights_in",
    )(*arrays)


COST = pl.CostEstimate(flops=2 * 256 * 7168 * 1024, transcendentals=0, bytes_accessed=0)


def gate_up_near(pieces, weights):
    return pl.pallas_call(
        near_kernel,
        out_shape=jax.ShapeDtypeStruct((4, 512, 256), F32),
        in_specs=[VMEM] * 7,
        out_specs=VMEM,
        cost_estimate=COST,
        compiler_params=pltpu.CompilerParams(vmem_limit_bytes=8 << 20),
        name="gate_up_near",
    )(*pieces, *weights)


def gate_up_far(expert, pieces, weights, near_x2, acc):
    return pl.pallas_call(
        far_kernel,
        out_shape=(
            jax.ShapeDtypeStruct((512, 512), BF16),
            jax.ShapeDtypeStruct((8, INFO), F32),
        ),
        in_specs=[SMEM] + [VMEM] * 9,
        out_specs=(VMEM, VMEM),
        scratch_shapes=[pltpu.VMEM((4, 512, 256), F32)],
        cost_estimate=COST,
        compiler_params=pltpu.CompilerParams(vmem_limit_bytes=10 << 20),
        name="gate_up_far",
    )(expert, *pieces, *weights, near_x2, acc)


def down_kernel(colour, far, hidden, own, other, out):
    cols = slice(COL_CUTS[colour], COL_CUTS[colour + 1])
    blocks = [canonical(colour, q + (4 if far else 0)) for q in range(4)]
    lhs = jnp.concatenate([hidden[64 * s : 64 * s + 64, :] for s in blocks], axis=0)
    total = jnp.dot(lhs[:, :256], own[:, cols], preferred_element_type=F32)
    total += jnp.dot(lhs[:, 256:], other[:, cols], preferred_element_type=F32)
    out[...] = total.astype(out.dtype)


def down_part(colour, far, hidden, own, other):
    width = COL_CUTS[colour + 1] - COL_CUTS[colour]
    return pl.pallas_call(
        functools.partial(down_kernel, colour, far),
        out_shape=jax.ShapeDtypeStruct((256, width), BF16 if far else F32),
        in_specs=[VMEM] * 3,
        out_specs=VMEM,
        cost_estimate=pl.CostEstimate(
            flops=2 * 256 * 512 * width, transcendentals=0, bytes_accessed=0
        ),
        compiler_params=pltpu.CompilerParams(vmem_limit_bytes=6 << 20),
    )(hidden, own, other)


def layer(
    tokens, expert_ids, slot_ids, route_weight, gate_weight, up_weight, down_weight, expert_bias
):
    experts = lax.axis_size("gx") * lax.axis_size("gy")
    devices = experts * lax.axis_size(GZ)
    tok_rows, width = tokens.shape
    route_count = expert_ids.shape[1]
    own_expert = lax.axis_index("gx") * lax.axis_size("gy") + lax.axis_index("gy")

    gate_own, up_own, down_own = gate_weight[0], up_weight[0], down_weight[0]
    gate_far, up_far, down_far = partner(gate_own), partner(up_own), partner(down_own)
    gate_own, gate_far, up_own, up_far = in_vmem(gate_own, gate_far, up_own, up_far)
    down_own, down_far = in_vmem(down_own, down_far)
    gate_ups = (gate_own, gate_far, up_own, up_far)

    rows = rows_of(tokens, expert_ids, route_weight, experts)
    rows = jnp.concatenate([rows] + [direct(rows, hops_of(n)) for n in range(1, 8)], axis=0)
    ends = (*CUTS[:3], width + INFO)
    pieces = [rows[:, ends[i] : ends[i + 1]] for i in range(3)]
    for step in range(2):
        pieces = [
            jnp.concatenate([p, exchange(p, LATE[i][step])], axis=0) for i, p in enumerate(pieces)
        ]
    far_pieces = [exchange(p, LATE[i][2]) for i, p in enumerate(pieces)]

    acc = gate_up_near(pieces, gate_ups)
    expert = jnp.full((1,), own_expert, jnp.int32)
    hidden, marks = gate_up_far(expert, far_pieces, gate_ups, pieces[2], acc)

    sent = [down_part(i, True, hidden, down_own, down_far) for i in range(3)]
    kept = []
    for i in range(3):
        kept.append(down_part(i, False, hidden, down_own, down_far))
    for step in (2, 1, 0):
        got = []
        for i in range(3):
            got.append(exchange(sent[i], LATE[i][step]))
        totals = [kept[i] + got[i].astype(F32) for i in range(3)]
        half = totals[0].shape[0] // 2
        if step:
            sent = [t[half:].astype(BF16) for t in totals]
            kept = [t[:half] for t in totals]
    total = jnp.concatenate(totals, axis=1)
    combined = total[:tok_rows]
    for n in range(1, 8):
        block = total[n * tok_rows : (n + 1) * tok_rows].astype(BF16)
        combined = combined + direct(block, hops_of(n)).astype(F32)

    half_load = jnp.sum(marks, axis=0)[experts : 2 * experts].astype(jnp.int32)
    other_load = partner(half_load)
    expert_load = half_load + other_load
    mean_load = tok_rows * devices * route_count // experts
    new_bias = expert_bias + bias_rate * jnp.sign((mean_load - expert_load).astype(F32))
    return (combined.astype(BF16), expert_load, new_bias)


def solution(mesh):
    finer = Mesh(mesh.devices.reshape(mesh.shape["gx"], mesh.shape["gy"], 4, 2), AXES)
    return jax.shard_map(
        layer,
        mesh=finer,
        in_specs=(
            P(AXES, None),
            P(AXES, None),
            P(AXES, None),
            P(AXES, None),
            P(("gx", "gy"), None, GZ),
            P(("gx", "gy"), None, GZ),
            P(("gx", "gy"), GZ, None),
            P(),
        ),
        out_specs=(P(AXES, None), P(), P()),
        check_vma=False,
    )
```

```python
import functools

import jax
import jax.numpy as jnp
from jax import lax
from jax.experimental import pallas as pl
from jax.experimental.pallas import tpu as pltpu
from jax.sharding import Mesh
from jax.sharding import PartitionSpec as P

AXES = ("gx", "gy", "gz_0", "gz_1")
GZ = ("gz_0", "gz_1")
X, Y, Z = "gz_0", "gx", "gy"
EARLY = (X, Y, Z)
LATE = ((X, Y, Z), (Y, Z, X), (Z, X, Y))
INFO = 128
CUTS = (0, 2560, 4864, 7168)
COL_CUTS = (0, 2432, 4864, 7168)
BF16 = jnp.bfloat16
F32 = jnp.float32

bias_rate = 0.001


def exchange(value, axis):
    masks = (3, 1)
    pairs = [(2 * i + c, 2 * (i ^ masks[c]) + c) for i in range(4) for c in range(2)]
    return lax.ppermute(value, (axis, "gz_1"), pairs)


def direct(value, hops):
    masks = (1, 3)
    pairs = []
    for a in range(4):
        for b in range(4):
            for x in range(4):
                for c in range(2):
                    m = masks[c]
                    far = (
                        a ^ (m if Y in hops else 0),
                        b ^ (m if Z in hops else 0),
                        x ^ (m if X in hops else 0),
                    )
                    here = ((a * 4 + b) * 4 + x) * 2 + c
                    pairs.append((here, ((far[0] * 4 + far[1]) * 4 + far[2]) * 2 + c))
    return lax.ppermute(value, AXES, pairs)


def hops_of(n):
    return [axis for k, axis in enumerate(EARLY) if n >> k & 1]


def partner(value):
    return lax.ppermute(value, "gz_1", [(0, 1), (1, 0)])


def canonical(colour, place):
    bits = {LATE[colour][k]: place >> k & 1 for k in range(3)}
    return sum(bits[LATE[0][k]] << k for k in range(3))


VMEM = pl.BlockSpec(memory_space=pltpu.VMEM)
SMEM = pl.BlockSpec(memory_space=pltpu.SMEM)


def rows_kernel(experts, tokens, ids_in, weights_in, out, ids, weights, sem):
    width = tokens.shape[1]
    copies = (
        pltpu.make_async_copy(ids_in, ids, sem.at[0]),
        pltpu.make_async_copy(weights_in, weights, sem.at[1]),
        pltpu.make_async_copy(tokens, out.at[:, pl.ds(0, width)], sem.at[2]),
    )
    for c in copies:
        c.start()
    copies[0].wait()
    copies[1].wait()
    lane = lax.broadcasted_iota(jnp.int32, (tokens.shape[0], INFO), 1)
    info = jnp.zeros((tokens.shape[0], INFO), F32)
    for k in range(ids.shape[1]):
        chosen = ids[:, k : k + 1]
        info += jnp.where(lane == chosen, weights[:, k : k + 1].astype(F32), 0.0)
        info += jnp.where(lane == chosen + experts, 1.0, 0.0)
    out[:, width:] = info.astype(BF16)
    copies[2].wait()


def rows_of(tokens, ids, weights, experts):
    rows, width = tokens.shape
    return pl.pallas_call(
        functools.partial(rows_kernel, experts),
        out_shape=jax.ShapeDtypeStruct((rows, width + INFO), BF16),
        in_specs=[pl.BlockSpec(memory_space=pltpu.HBM)] * 3,
        out_specs=VMEM,
        scratch_shapes=[
            pltpu.VMEM(ids.shape, ids.dtype),
            pltpu.VMEM(weights.shape, weights.dtype),
            pltpu.SemaphoreType.DMA((3,)),
        ],
        compiler_params=pltpu.CompilerParams(vmem_limit_bytes=4 << 20),
        name="token_rows",
    )(tokens, ids, weights)


def near_kernel(x0, x1, x2, w0, w1, w2, w3, acc):
    for i, x in enumerate((x0, x1, x2)):
        width = CUTS[i + 1] - CUTS[i]
        places = [canonical(i, q) for q in range(4)]
        for j, w in enumerate((w0, w1, w2, w3)):
            part = jnp.dot(
                x[:, :width], w[CUTS[i] : CUTS[i + 1], :], preferred_element_type=F32
            )
            for q, s in enumerate(places):
                rows = part[64 * q : 64 * q + 64]
                if i == 0:
                    acc[j, 64 * s : 64 * s + 64, :] = rows
                else:
                    acc[j, 64 * s : 64 * s + 64, :] += rows
            if i == 0:
                for s in range(8):
                    if s not in places:
                        acc[j, 64 * s : 64 * s + 64, :] = jnp.zeros((64, 256), F32)


def far_part_kernel(colour, x, w0, w1, w2, w3, out):
    rows = slice(CUTS[colour], CUTS[colour + 1])
    width = CUTS[colour + 1] - CUTS[colour]
    for j, w in enumerate((w0, w1, w2, w3)):
        out[j] = jnp.dot(x[:, :width], w[rows, :], preferred_element_type=F32)


def far_last_kernel(
    expert, x0, w0, w1, w2, w3, part1, part2, near_x2, far_x2, acc_in, hidden, marks, acc
):
    far_places = [{canonical(i, q + 4): 64 * q for q in range(4)} for i in range(3)]
    for j, w in enumerate((w0, w1, w2, w3)):
        mine = jnp.dot(x0[...], w[: CUTS[1], :], preferred_element_type=F32)
        for s in range(8):
            rows = acc_in[j, 64 * s : 64 * s + 64, :]
            if s in far_places[0]:
                at = far_places[0][s]
                rows += mine[at : at + 64]
            for i, part in ((1, part1), (2, part2)):
                if s in far_places[i]:
                    at = far_places[i][s]
                    rows += part[j, at : at + 64, :]
            acc[j, 64 * s : 64 * s + 64, :] = rows
    lane = lax.broadcasted_iota(jnp.int32, (64, INFO), 1)
    sums = jnp.zeros((8, INFO), F32)
    for place in range(8):
        s = canonical(2, place)
        source = near_x2 if place < 4 else far_x2
        at = 64 * (place % 4)
        info = source[at : at + 64, CUTS[3] - CUTS[2] :].astype(F32)
        sums += jnp.sum(info.reshape(8, 8, INFO), axis=0)
        scale = jnp.sum(jnp.where(lane == expert[0], info, 0.0), axis=1, keepdims=True)
        for part in range(2):
            g = acc[part, 64 * s : 64 * s + 64, :]
            u = acc[part + 2, 64 * s : 64 * s + 64, :]
            h = g / (1.0 + jnp.exp(-g)) * u * scale
            hidden[64 * s : 64 * s + 64, 256 * part : 256 * part + 256] = h.astype(BF16)
    marks[...] = jnp.sum(sums, axis=0, keepdims=True).astype(jnp.int32)


def load_kernel(*refs):
    count = (len(refs) - 1) // 2
    sem = refs[-1]
    copies = [
        pltpu.make_async_copy(refs[k], refs[count + k], sem.at[k]) for k in range(count)
    ]
    for c in copies:
        c.start()
    for c in copies:
        c.wait()


def in_vmem(*arrays):
    return pl.pallas_call(
        load_kernel,
        out_shape=tuple(jax.ShapeDtypeStruct(a.shape, a.dtype) for a in arrays),
        in_specs=[pl.BlockSpec(memory_space=pl.ANY)] * len(arrays),
        out_specs=(VMEM,) * len(arrays),
        scratch_shapes=[pltpu.SemaphoreType.DMA((len(arrays),))],
        compiler_params=pltpu.CompilerParams(vmem_limit_bytes=4 << 20),
        cost_estimate=pl.CostEstimate(flops=8 << 30, transcendentals=0, bytes_accessed=0),
        name="weights_in",
    )(*arrays)


def cost(parts):
    return pl.CostEstimate(
        flops=2 * 256 * 2389 * 1024 * parts, transcendentals=0, bytes_accessed=0
    )


def gate_up_near(pieces, weights):
    return pl.pallas_call(
        near_kernel,
        out_shape=jax.ShapeDtypeStruct((4, 512, 256), F32),
        in_specs=[VMEM] * 7,
        out_specs=VMEM,
        cost_estimate=cost(3),
        compiler_params=pltpu.CompilerParams(vmem_limit_bytes=8 << 20),
        name="gate_up_near",
    )(*pieces, *weights)


def gate_up_far_part(colour, piece, weights):
    return pl.pallas_call(
        functools.partial(far_part_kernel, colour),
        out_shape=jax.ShapeDtypeStruct((4, 256, 256), F32),
        in_specs=[VMEM] * 5,
        out_specs=VMEM,
        cost_estimate=cost(1),
        compiler_params=pltpu.CompilerParams(vmem_limit_bytes=6 << 20),
    )(piece, *weights)


def gate_up_last(expert, piece, weights, parts, near_x2, far_x2, acc):
    return pl.pallas_call(
        far_last_kernel,
        out_shape=(
            jax.ShapeDtypeStruct((512, 512), BF16),
            jax.ShapeDtypeStruct((1, INFO), jnp.int32),
        ),
        in_specs=[SMEM] + [VMEM] * 10,
        out_specs=(VMEM, VMEM),
        scratch_shapes=[pltpu.VMEM((4, 512, 256), F32)],
        cost_estimate=cost(1),
        compiler_params=pltpu.CompilerParams(vmem_limit_bytes=10 << 20),
        name="gate_up_far_0",
    )(expert, piece, *weights, *parts, near_x2, far_x2, acc)


def down_kernel(colour, far, hidden, own, other, out):
    cols = slice(COL_CUTS[colour], COL_CUTS[colour + 1])
    blocks = [canonical(colour, q + (4 if far else 0)) for q in range(4)]
    lhs = jnp.concatenate([hidden[64 * s : 64 * s + 64, :] for s in blocks], axis=0)
    total = jnp.dot(lhs[:, :256], own[:, cols], preferred_element_type=F32)
    total += jnp.dot(lhs[:, 256:], other[:, cols], preferred_element_type=F32)
    out[...] = total.astype(out.dtype)


def down_part(colour, far, hidden, own, other):
    width = COL_CUTS[colour + 1] - COL_CUTS[colour]
    return pl.pallas_call(
        functools.partial(down_kernel, colour, far),
        out_shape=jax.ShapeDtypeStruct((256, width), BF16 if far else F32),
        in_specs=[VMEM] * 3,
        out_specs=VMEM,
        cost_estimate=pl.CostEstimate(
            flops=2 * 256 * 512 * width, transcendentals=0, bytes_accessed=0
        ),
        compiler_params=pltpu.CompilerParams(vmem_limit_bytes=6 << 20),
    )(hidden, own, other)


def layer(
    tokens, expert_ids, slot_ids, route_weight, gate_weight, up_weight, down_weight, expert_bias
):
    experts = lax.axis_size("gx") * lax.axis_size("gy")
    devices = experts * lax.axis_size(GZ)
    tok_rows, width = tokens.shape
    route_count = expert_ids.shape[1]
    own_expert = lax.axis_index("gx") * lax.axis_size("gy") + lax.axis_index("gy")

    gate_own, up_own, down_own = gate_weight[0], up_weight[0], down_weight[0]
    gate_far = partner(gate_own)
    up_far = partner(up_own)
    down_far = partner(down_own)
    gate_own, gate_far, up_own, up_far = in_vmem(gate_own, gate_far, up_own, up_far)
    down_own, down_far = in_vmem(down_own, down_far)
    gate_ups = (gate_own, gate_far, up_own, up_far)

    rows = rows_of(tokens, expert_ids, route_weight, experts)
    rows = jnp.concatenate([rows] + [direct(rows, hops_of(n)) for n in range(1, 8)], axis=0)
    ends = (*CUTS[:3], width + INFO)
    pieces = [rows[:, ends[i] : ends[i + 1]] for i in range(3)]
    for step in range(3):
        far_pieces = []
        for i, p in enumerate(pieces):
            far_pieces.append(exchange(p, LATE[i][step]))
        if step < 2:
            pieces = [jnp.concatenate(pair, axis=0) for pair in zip(pieces, far_pieces)]

    acc = gate_up_near(pieces, gate_ups)
    expert = jnp.full((1,), own_expert, jnp.int32)
    parts = [gate_up_far_part(i, far_pieces[i], gate_ups) for i in (1, 2)]
    hidden, marks = gate_up_last(
        expert, far_pieces[0], gate_ups, parts, pieces[2], far_pieces[2], acc
    )

    sent = [down_part(i, True, hidden, down_own, down_far) for i in range(3)]
    kept = []
    for i in range(3):
        kept.append(down_part(i, False, hidden, down_own, down_far))
    for step in (2, 1, 0):
        got = []
        for i in range(3):
            got.append(exchange(sent[i], LATE[i][step]))
        totals = [kept[i] + got[i].astype(F32) for i in range(3)]
        half = totals[0].shape[0] // 2
        if step:
            sent = [t[half:].astype(BF16) for t in totals]
            kept = [t[:half] for t in totals]
    total = jnp.concatenate(totals, axis=1)
    combined = total[:tok_rows]
    for n in range(1, 8):
        block = total[n * tok_rows : (n + 1) * tok_rows].astype(BF16)
        combined = combined + direct(block, hops_of(n)).astype(F32)

    other_marks = partner(marks)
    expert_load = (marks + other_marks)[0, experts : 2 * experts]
    mean_load = tok_rows * devices * route_count // experts
    new_bias = expert_bias + bias_rate * jnp.sign((mean_load - expert_load).astype(F32))
    return (combined.astype(BF16), expert_load, new_bias)


def solution(mesh):
    finer = Mesh(mesh.devices.reshape(mesh.shape["gx"], mesh.shape["gy"], 4, 2), AXES)
    return jax.shard_map(
        layer,
        mesh=finer,
        in_specs=(
            P(AXES, None),
            P(AXES, None),
            P(AXES, None),
            P(AXES, None),
            P(("gx", "gy"), None, GZ),
            P(("gx", "gy"), None, GZ),
            P(("gx", "gy"), GZ, None),
            P(),
        ),
        out_specs=(P(AXES, None), P(), P()),
        check_vma=False,
    )
```

```python
import functools

import jax
import jax.numpy as jnp
from jax import lax
from jax.experimental import pallas as pl
from jax.experimental.pallas import tpu as pltpu
from jax.sharding import Mesh
from jax.sharding import PartitionSpec as P

AXES = ("gx", "gy", "gz_0", "gz_1")
GZ = ("gz_0", "gz_1")
X, Y, Z = "gz_0", "gx", "gy"
EARLY = (X, Y, Z)
LATE = ((X, Y, Z), (Y, Z, X), (Z, X, Y))
INFO = 128
CUTS = (0, 2560, 4864, 7168)
COL_CUTS = (0, 2432, 4864, 7168)
BF16 = jnp.bfloat16
F32 = jnp.float32

bias_rate = 0.001


def exchange(value, axis):
    masks = (3, 1)
    pairs = [(2 * i + c, 2 * (i ^ masks[c]) + c) for i in range(4) for c in range(2)]
    return lax.ppermute(value, (axis, "gz_1"), pairs)


def direct(value, hops):
    masks = (1, 3)
    pairs = []
    for a in range(4):
        for b in range(4):
            for x in range(4):
                for c in range(2):
                    m = masks[c]
                    far = (
                        a ^ (m if Y in hops else 0),
                        b ^ (m if Z in hops else 0),
                        x ^ (m if X in hops else 0),
                    )
                    here = ((a * 4 + b) * 4 + x) * 2 + c
                    pairs.append((here, ((far[0] * 4 + far[1]) * 4 + far[2]) * 2 + c))
    return lax.ppermute(value, AXES, pairs)


def hops_of(n):
    return [axis for k, axis in enumerate(EARLY) if n >> k & 1]


def partner(value):
    return lax.ppermute(value, "gz_1", [(0, 1), (1, 0)])


def canonical(colour, place):
    bits = {LATE[colour][k]: place >> k & 1 for k in range(3)}
    return sum(bits[LATE[0][k]] << k for k in range(3))


VMEM = pl.BlockSpec(memory_space=pltpu.VMEM)
SMEM = pl.BlockSpec(memory_space=pltpu.SMEM)


def rows_kernel(experts, tokens, ids_in, weights_in, out, ids, weights, sem):
    width = tokens.shape[1]
    copies = (
        pltpu.make_async_copy(ids_in, ids, sem.at[0]),
        pltpu.make_async_copy(weights_in, weights, sem.at[1]),
        pltpu.make_async_copy(tokens, out.at[:, pl.ds(0, width)], sem.at[2]),
    )
    for c in copies:
        c.start()
    copies[0].wait()
    copies[1].wait()
    lane = lax.broadcasted_iota(jnp.int32, (tokens.shape[0], INFO), 1)
    info = jnp.zeros((tokens.shape[0], INFO), F32)
    for k in range(ids.shape[1]):
        chosen = ids[:, k : k + 1]
        info += jnp.where(lane == chosen, weights[:, k : k + 1].astype(F32), 0.0)
        info += jnp.where(lane == chosen + experts, 1.0, 0.0)
    out[:, width:] = info.astype(BF16)
    copies[2].wait()


def rows_of(tokens, ids, weights, experts):
    rows, width = tokens.shape
    return pl.pallas_call(
        functools.partial(rows_kernel, experts),
        out_shape=jax.ShapeDtypeStruct((rows, width + INFO), BF16),
        in_specs=[pl.BlockSpec(memory_space=pltpu.HBM)] * 3,
        out_specs=VMEM,
        scratch_shapes=[
            pltpu.VMEM(ids.shape, ids.dtype),
            pltpu.VMEM(weights.shape, weights.dtype),
            pltpu.SemaphoreType.DMA((3,)),
        ],
        compiler_params=pltpu.CompilerParams(vmem_limit_bytes=4 << 20),
        name="token_rows",
    )(tokens, ids, weights)


def near_kernel(x0, x1, x2, w0, w1, w2, w3, acc):
    for i, x in enumerate((x0, x1, x2)):
        width = CUTS[i + 1] - CUTS[i]
        places = [canonical(i, q) for q in range(4)]
        for j, w in enumerate((w0, w1, w2, w3)):
            part = jnp.dot(
                x[:, :width], w[CUTS[i] : CUTS[i + 1], :], preferred_element_type=F32
            )
            for q, s in enumerate(places):
                rows = part[64 * q : 64 * q + 64]
                if i == 0:
                    acc[j, 64 * s : 64 * s + 64, :] = rows
                else:
                    acc[j, 64 * s : 64 * s + 64, :] += rows
            if i == 0:
                for s in range(8):
                    if s not in places:
                        acc[j, 64 * s : 64 * s + 64, :] = jnp.zeros((64, 256), F32)


def far_part_kernel(colour, x, w0, w1, w2, w3, out):
    rows = slice(CUTS[colour], CUTS[colour + 1])
    width = CUTS[colour + 1] - CUTS[colour]
    for j, w in enumerate((w0, w1, w2, w3)):
        out[j] = jnp.dot(x[:, :width], w[rows, :], preferred_element_type=F32)


def far_last_kernel(
    expert, x0, w0, w1, w2, w3, part1, part2, near_x2, far_x2, acc_in, hidden, marks, acc
):
    far_places = [{canonical(i, q + 4): 64 * q for q in range(4)} for i in range(3)]
    for j, w in enumerate((w0, w1, w2, w3)):
        mine = jnp.dot(x0[...], w[: CUTS[1], :], preferred_element_type=F32)
        for s in range(8):
            rows = acc_in[j, 64 * s : 64 * s + 64, :]
            if s in far_places[0]:
                at = far_places[0][s]
                rows += mine[at : at + 64]
            for i, part in ((1, part1), (2, part2)):
                if s in far_places[i]:
                    at = far_places[i][s]
                    rows += part[j, at : at + 64, :]
            acc[j, 64 * s : 64 * s + 64, :] = rows
    lane = lax.broadcasted_iota(jnp.int32, (64, INFO), 1)
    sums = jnp.zeros((8, INFO), F32)
    for place in range(8):
        s = canonical(2, place)
        source = near_x2 if place < 4 else far_x2
        at = 64 * (place % 4)
        info = source[at : at + 64, CUTS[3] - CUTS[2] :].astype(F32)
        sums += jnp.sum(info.reshape(8, 8, INFO), axis=0)
        scale = jnp.sum(jnp.where(lane == expert[0], info, 0.0), axis=1, keepdims=True)
        for part in range(2):
            g = acc[part, 64 * s : 64 * s + 64, :]
            u = acc[part + 2, 64 * s : 64 * s + 64, :]
            h = g / (1.0 + jnp.exp(-g)) * u * scale
            hidden[64 * s : 64 * s + 64, 256 * part : 256 * part + 256] = h.astype(BF16)
    marks[...] = jnp.sum(sums, axis=0, keepdims=True).astype(jnp.int32)


def load_kernel(*refs):
    count = (len(refs) - 1) // 2
    sem = refs[-1]
    copies = [
        pltpu.make_async_copy(refs[k], refs[count + k], sem.at[k]) for k in range(count)
    ]
    for c in copies:
        c.start()
    for c in copies:
        c.wait()


def in_vmem(*arrays):
    return pl.pallas_call(
        load_kernel,
        out_shape=tuple(jax.ShapeDtypeStruct(a.shape, a.dtype) for a in arrays),
        in_specs=[pl.BlockSpec(memory_space=pl.ANY)] * len(arrays),
        out_specs=(VMEM,) * len(arrays),
        scratch_shapes=[pltpu.SemaphoreType.DMA((len(arrays),))],
        compiler_params=pltpu.CompilerParams(vmem_limit_bytes=4 << 20),
        cost_estimate=pl.CostEstimate(flops=8 << 30, transcendentals=0, bytes_accessed=0),
        name="weights_in",
    )(*arrays)


def cost(parts):
    return pl.CostEstimate(
        flops=2 * 256 * 2389 * 1024 * parts, transcendentals=0, bytes_accessed=0
    )


def gate_up_near(pieces, weights):
    return pl.pallas_call(
        near_kernel,
        out_shape=jax.ShapeDtypeStruct((4, 512, 256), F32),
        in_specs=[VMEM] * 7,
        out_specs=VMEM,
        cost_estimate=cost(3),
        compiler_params=pltpu.CompilerParams(vmem_limit_bytes=8 << 20),
        name="gate_up_near",
    )(*pieces, *weights)


def gate_up_far_part(colour, piece, weights):
    return pl.pallas_call(
        functools.partial(far_part_kernel, colour),
        out_shape=jax.ShapeDtypeStruct((4, 256, 256), F32),
        in_specs=[VMEM] * 5,
        out_specs=VMEM,
        cost_estimate=cost(1),
        compiler_params=pltpu.CompilerParams(vmem_limit_bytes=6 << 20),
    )(piece, *weights)


def gate_up_last(expert, piece, weights, parts, near_x2, far_x2, acc):
    return pl.pallas_call(
        far_last_kernel,
        out_shape=(
            jax.ShapeDtypeStruct((512, 512), BF16),
            jax.ShapeDtypeStruct((1, INFO), jnp.int32),
        ),
        in_specs=[SMEM] + [VMEM] * 10,
        out_specs=(VMEM, VMEM),
        scratch_shapes=[pltpu.VMEM((4, 512, 256), F32)],
        cost_estimate=cost(1),
        compiler_params=pltpu.CompilerParams(vmem_limit_bytes=10 << 20),
        name="gate_up_far_0",
    )(expert, piece, *weights, *parts, near_x2, far_x2, acc)


def down_kernel(colour, far, hidden, own, other, out):
    cols = slice(COL_CUTS[colour], COL_CUTS[colour + 1])
    blocks = [canonical(colour, q + (4 if far else 0)) for q in range(4)]
    lhs = jnp.concatenate([hidden[64 * s : 64 * s + 64, :] for s in blocks], axis=0)
    total = jnp.dot(lhs[:, :256], own[:, cols], preferred_element_type=F32)
    total += jnp.dot(lhs[:, 256:], other[:, cols], preferred_element_type=F32)
    out[...] = total.astype(out.dtype)


def down_part(colour, far, hidden, own, other):
    width = COL_CUTS[colour + 1] - COL_CUTS[colour]
    return pl.pallas_call(
        functools.partial(down_kernel, colour, far),
        out_shape=jax.ShapeDtypeStruct((256, width), BF16 if far else F32),
        in_specs=[VMEM] * 3,
        out_specs=VMEM,
        cost_estimate=pl.CostEstimate(
            flops=2 * 256 * 512 * width, transcendentals=0, bytes_accessed=0
        ),
        compiler_params=pltpu.CompilerParams(vmem_limit_bytes=6 << 20),
    )(hidden, own, other)


def layer(
    tokens, expert_ids, slot_ids, route_weight, gate_weight, up_weight, down_weight, expert_bias
):
    experts = lax.axis_size("gx") * lax.axis_size("gy")
    devices = experts * lax.axis_size(GZ)
    tok_rows, width = tokens.shape
    route_count = expert_ids.shape[1]
    own_expert = lax.axis_index("gx") * lax.axis_size("gy") + lax.axis_index("gy")

    gate_own, up_own, down_own = gate_weight[0], up_weight[0], down_weight[0]
    gate_far = partner(gate_own)
    up_far = partner(up_own)
    down_far = partner(down_own)
    gate_own, gate_far, up_own, up_far = in_vmem(gate_own, gate_far, up_own, up_far)
    down_own, down_far = in_vmem(down_own, down_far)
    gate_ups = (gate_own, gate_far, up_own, up_far)

    rows = rows_of(tokens, expert_ids, route_weight, experts)
    blocks = [rows]
    for n in range(1, 8):
        blocks.append(direct(rows, hops_of(n)))
    rows = jnp.concatenate(blocks, axis=0)
    ends = (*CUTS[:3], width + INFO)
    pieces = [rows[:, ends[i] : ends[i + 1]] for i in range(3)]
    for step in range(3):
        far_pieces = []
        for i, p in enumerate(pieces):
            far_pieces.append(exchange(p, LATE[i][step]))
        if step < 2:
            pieces = [jnp.concatenate(pair, axis=0) for pair in zip(pieces, far_pieces)]

    acc = gate_up_near(pieces, gate_ups)
    expert = jnp.full((1,), own_expert, jnp.int32)
    parts = [gate_up_far_part(i, far_pieces[i], gate_ups) for i in (1, 2)]
    hidden, marks = gate_up_last(
        expert, far_pieces[0], gate_ups, parts, pieces[2], far_pieces[2], acc
    )

    sent = [down_part(i, True, hidden, down_own, down_far) for i in range(3)]
    kept = []
    for i in range(3):
        kept.append(down_part(i, False, hidden, down_own, down_far))
    for step in (2, 1, 0):
        got = []
        for i in range(3):
            got.append(exchange(sent[i], LATE[i][step]))
        totals = [kept[i] + got[i].astype(F32) for i in range(3)]
        half = totals[0].shape[0] // 2
        if step:
            sent = [t[half:].astype(BF16) for t in totals]
            kept = [t[:half] for t in totals]
    total = jnp.concatenate(totals, axis=1)
    combined = total[:tok_rows]
    for n in range(1, 8):
        block = total[n * tok_rows : (n + 1) * tok_rows].astype(BF16)
        block = direct(block, hops_of(n))
        combined = combined + block.astype(F32)

    other_marks = partner(marks)
    expert_load = (marks + other_marks)[0, experts : 2 * experts]
    mean_load = tok_rows * devices * route_count // experts
    new_bias = expert_bias + bias_rate * jnp.sign((mean_load - expert_load).astype(F32))
    return (combined.astype(BF16), expert_load, new_bias)


def solution(mesh):
    finer = Mesh(mesh.devices.reshape(mesh.shape["gx"], mesh.shape["gy"], 4, 2), AXES)
    return jax.shard_map(
        layer,
        mesh=finer,
        in_specs=(
            P(AXES, None),
            P(AXES, None),
            P(AXES, None),
            P(AXES, None),
            P(("gx", "gy"), None, GZ),
            P(("gx", "gy"), None, GZ),
            P(("gx", "gy"), GZ, None),
            P(),
        ),
        out_specs=(P(AXES, None), P(), P()),
        check_vma=False,
    )
```

```python
import functools

import jax
import jax.numpy as jnp
from jax import lax
from jax.experimental import pallas as pl
from jax.experimental.pallas import tpu as pltpu
from jax.sharding import Mesh
from jax.sharding import PartitionSpec as P

AXES = ("gx", "gy", "gz_0", "gz_1")
GZ = ("gz_0", "gz_1")
X, Y, Z = "gz_0", "gx", "gy"
EARLY = (X, Y, Z)
LATE = ((X, Y, Z), (Y, Z, X), (Z, X, Y))
INFO = 128
CUTS = (0, 2432, 4864, 7168)
COL_CUTS = (0, 2432, 4864, 7168)
BF16 = jnp.bfloat16
F32 = jnp.float32

bias_rate = 0.001


def exchange(value, axis):
    masks = (3, 1)
    pairs = [(2 * i + c, 2 * (i ^ masks[c]) + c) for i in range(4) for c in range(2)]
    return lax.ppermute(value, (axis, "gz_1"), pairs)


def direct(value, hops):
    masks = (1, 3)
    pairs = []
    for a in range(4):
        for b in range(4):
            for x in range(4):
                for c in range(2):
                    m = masks[c]
                    far = (
                        a ^ (m if Y in hops else 0),
                        b ^ (m if Z in hops else 0),
                        x ^ (m if X in hops else 0),
                    )
                    here = ((a * 4 + b) * 4 + x) * 2 + c
                    pairs.append((here, ((far[0] * 4 + far[1]) * 4 + far[2]) * 2 + c))
    return lax.ppermute(value, AXES, pairs)


def hops_of(n):
    return [axis for k, axis in enumerate(EARLY) if n >> k & 1]


def partner(value):
    return lax.ppermute(value, "gz_1", [(0, 1), (1, 0)])


def canonical(colour, place):
    bits = {LATE[colour][k]: place >> k & 1 for k in range(3)}
    return sum(bits[LATE[0][k]] << k for k in range(3))


VMEM = pl.BlockSpec(memory_space=pltpu.VMEM)
SMEM = pl.BlockSpec(memory_space=pltpu.SMEM)


def rows_kernel(experts, tokens, ids_in, weights_in, out, ids, weights, sem):
    width = tokens.shape[1]
    copies = (
        pltpu.make_async_copy(ids_in, ids, sem.at[0]),
        pltpu.make_async_copy(weights_in, weights, sem.at[1]),
        pltpu.make_async_copy(tokens, out.at[:, pl.ds(0, width)], sem.at[2]),
    )
    for c in copies:
        c.start()
    copies[0].wait()
    copies[1].wait()
    lane = lax.broadcasted_iota(jnp.int32, (tokens.shape[0], INFO), 1)
    info = jnp.zeros((tokens.shape[0], INFO), F32)
    for k in range(ids.shape[1]):
        chosen = ids[:, k : k + 1]
        info += jnp.where(lane == chosen, weights[:, k : k + 1].astype(F32), 0.0)
        info += jnp.where(lane == chosen + experts, 1.0, 0.0)
    out[:, width:] = info.astype(BF16)
    copies[2].wait()


def rows_of(tokens, ids, weights, experts):
    rows, width = tokens.shape
    return pl.pallas_call(
        functools.partial(rows_kernel, experts),
        out_shape=jax.ShapeDtypeStruct((rows, width + INFO), BF16),
        in_specs=[pl.BlockSpec(memory_space=pltpu.HBM)] * 3,
        out_specs=VMEM,
        scratch_shapes=[
            pltpu.VMEM(ids.shape, ids.dtype),
            pltpu.VMEM(weights.shape, weights.dtype),
            pltpu.SemaphoreType.DMA((3,)),
        ],
        compiler_params=pltpu.CompilerParams(vmem_limit_bytes=4 << 20),
        name="token_rows",
    )(tokens, ids, weights)


def near_kernel(x0, x1, x2, w0, w1, w2, w3, acc):
    for i, x in enumerate((x0, x1, x2)):
        width = CUTS[i + 1] - CUTS[i]
        places = [canonical(i, q) for q in range(4)]
        for j, w in enumerate((w0, w1, w2, w3)):
            part = jnp.dot(
                x[:, :width], w[CUTS[i] : CUTS[i + 1], :], preferred_element_type=F32
            )
            for q, s in enumerate(places):
                rows = part[64 * q : 64 * q + 64]
                if i == 0:
                    acc[j, 64 * s : 64 * s + 64, :] = rows
                else:
                    acc[j, 64 * s : 64 * s + 64, :] += rows
            if i == 0:
                for s in range(8):
                    if s not in places:
                        acc[j, 64 * s : 64 * s + 64, :] = jnp.zeros((64, 256), F32)


def far_part_kernel(colour, x, w0, w1, w2, w3, out):
    rows = slice(CUTS[colour], CUTS[colour + 1])
    width = CUTS[colour + 1] - CUTS[colour]
    for j, w in enumerate((w0, w1, w2, w3)):
        out[j] = jnp.dot(x[:, :width], w[rows, :], preferred_element_type=F32)


def hidden_kernel(expert, part0, part1, part2, near_x2, x2, acc, hidden, marks):
    parts = (part0, part1, part2)
    far_places = [{canonical(i, q + 4): 64 * q for q in range(4)} for i in range(3)]

    def total(j, s):
        rows = acc[j, 64 * s : 64 * s + 64, :]
        for i in range(3):
            if s in far_places[i]:
                at = far_places[i][s]
                rows += parts[i][j, at : at + 64, :]
        return rows

    lane = lax.broadcasted_iota(jnp.int32, (64, INFO), 1)
    sums = jnp.zeros((8, INFO), F32)
    for place in range(8):
        s = canonical(2, place)
        source = near_x2 if place < 4 else x2
        at = 64 * (place % 4)
        info = source[at : at + 64, CUTS[3] - CUTS[2] :].astype(F32)
        sums += jnp.sum(info.reshape(8, 8, INFO), axis=0)
        scale = jnp.sum(jnp.where(lane == expert[0], info, 0.0), axis=1, keepdims=True)
        for part in range(2):
            g, u = total(part, s), total(part + 2, s)
            h = g / (1.0 + jnp.exp(-g)) * u * scale
            hidden[64 * s : 64 * s + 64, 256 * part : 256 * part + 256] = h.astype(BF16)
    marks[...] = jnp.sum(sums, axis=0, keepdims=True).astype(jnp.int32)


def load_kernel(*refs):
    count = (len(refs) - 1) // 2
    sem = refs[-1]
    copies = [
        pltpu.make_async_copy(refs[k], refs[count + k], sem.at[k]) for k in range(count)
    ]
    for c in copies:
        c.start()
    for c in copies:
        c.wait()


def in_vmem(*arrays):
    return pl.pallas_call(
        load_kernel,
        out_shape=tuple(jax.ShapeDtypeStruct(a.shape, a.dtype) for a in arrays),
        in_specs=[pl.BlockSpec(memory_space=pl.ANY)] * len(arrays),
        out_specs=(VMEM,) * len(arrays),
        scratch_shapes=[pltpu.SemaphoreType.DMA((len(arrays),))],
        compiler_params=pltpu.CompilerParams(vmem_limit_bytes=4 << 20),
        cost_estimate=pl.CostEstimate(flops=8 << 30, transcendentals=0, bytes_accessed=0),
        name="weights_in",
    )(*arrays)


def cost(parts):
    return pl.CostEstimate(
        flops=2 * 256 * 2389 * 1024 * parts, transcendentals=0, bytes_accessed=0
    )


def gate_up_near(pieces, weights):
    return pl.pallas_call(
        near_kernel,
        out_shape=jax.ShapeDtypeStruct((4, 512, 256), F32),
        in_specs=[VMEM] * 7,
        out_specs=VMEM,
        cost_estimate=cost(3),
        compiler_params=pltpu.CompilerParams(vmem_limit_bytes=8 << 20),
        name="gate_up_near",
    )(*pieces, *weights)


def gate_up_far_part(colour, piece, weights):
    return pl.pallas_call(
        functools.partial(far_part_kernel, colour),
        out_shape=jax.ShapeDtypeStruct((4, 256, 256), F32),
        in_specs=[VMEM] * 5,
        out_specs=VMEM,
        cost_estimate=cost(1),
        compiler_params=pltpu.CompilerParams(vmem_limit_bytes=6 << 20),
    )(piece, *weights)


def hidden_of(expert, parts, near_x2, far_x2, acc):
    return pl.pallas_call(
        hidden_kernel,
        out_shape=(
            jax.ShapeDtypeStruct((512, 512), BF16),
            jax.ShapeDtypeStruct((1, INFO), jnp.int32),
        ),
        in_specs=[SMEM] + [VMEM] * 6,
        out_specs=(VMEM, VMEM),
        cost_estimate=cost(1),
        compiler_params=pltpu.CompilerParams(vmem_limit_bytes=6 << 20),
        name="hidden",
    )(expert, *parts, near_x2, far_x2, acc)


def down_kernel(colour, far, hidden, own, other, out):
    cols = slice(COL_CUTS[colour], COL_CUTS[colour + 1])
    blocks = [canonical(colour, q + (4 if far else 0)) for q in range(4)]
    lhs = jnp.concatenate([hidden[64 * s : 64 * s + 64, :] for s in blocks], axis=0)
    total = jnp.dot(lhs[:, :256], own[:, cols], preferred_element_type=F32)
    total += jnp.dot(lhs[:, 256:], other[:, cols], preferred_element_type=F32)
    out[...] = total.astype(out.dtype)


def down_part(colour, far, hidden, own, other):
    width = COL_CUTS[colour + 1] - COL_CUTS[colour]
    return pl.pallas_call(
        functools.partial(down_kernel, colour, far),
        out_shape=jax.ShapeDtypeStruct((256, width), BF16 if far else F32),
        in_specs=[VMEM] * 3,
        out_specs=VMEM,
        cost_estimate=pl.CostEstimate(
            flops=2 * 256 * 512 * width, transcendentals=0, bytes_accessed=0
        ),
        compiler_params=pltpu.CompilerParams(vmem_limit_bytes=6 << 20),
    )(hidden, own, other)


def layer(
    tokens, expert_ids, slot_ids, route_weight, gate_weight, up_weight, down_weight, expert_bias
):
    experts = lax.axis_size("gx") * lax.axis_size("gy")
    devices = experts * lax.axis_size(GZ)
    tok_rows, width = tokens.shape
    route_count = expert_ids.shape[1]
    own_expert = lax.axis_index("gx") * lax.axis_size("gy") + lax.axis_index("gy")

    gate_own, up_own, down_own = gate_weight[0], up_weight[0], down_weight[0]
    gate_far = partner(gate_own)
    up_far = partner(up_own)
    down_far = partner(down_own)
    gate_own, gate_far, up_own, up_far = in_vmem(gate_own, gate_far, up_own, up_far)
    down_own, down_far = in_vmem(down_own, down_far)
    gate_ups = (gate_own, gate_far, up_own, up_far)

    rows = rows_of(tokens, expert_ids, route_weight, experts)
    blocks = [rows]
    for n in range(1, 8):
        blocks.append(direct(rows, hops_of(n)))
    rows = jnp.concatenate(blocks, axis=0)
    ends = (*CUTS[:3], width + INFO)
    pieces = [rows[:, ends[i] : ends[i + 1]] for i in range(3)]
    for step in range(3):
        far_pieces = []
        for i, p in enumerate(pieces):
            far_pieces.append(exchange(p, LATE[i][step]))
        if step < 2:
            pieces = [jnp.concatenate(pair, axis=0) for pair in zip(pieces, far_pieces)]

    acc = gate_up_near(pieces, gate_ups)
    expert = jnp.full((1,), own_expert, jnp.int32)
    parts = [gate_up_far_part(i, far_pieces[i], gate_ups) for i in range(3)]
    hidden, marks = hidden_of(expert, parts, pieces[2], far_pieces[2], acc)

    sent = [down_part(i, True, hidden, down_own, down_far) for i in range(3)]
    kept = []
    for i in range(3):
        kept.append(down_part(i, False, hidden, down_own, down_far))
    for step in (2, 1, 0):
        got = []
        for i in range(3):
            got.append(exchange(sent[i], LATE[i][step]))
        totals = [kept[i] + got[i].astype(F32) for i in range(3)]
        half = totals[0].shape[0] // 2
        if step:
            sent = [t[half:].astype(BF16) for t in totals]
            kept = [t[:half] for t in totals]
    total = jnp.concatenate(totals, axis=1)
    combined = total[:tok_rows]
    for n in range(1, 8):
        block = total[n * tok_rows : (n + 1) * tok_rows].astype(BF16)
        block = direct(block, hops_of(n))
        combined = combined + block.astype(F32)

    other_marks = partner(marks)
    expert_load = (marks + other_marks)[0, experts : 2 * experts]
    mean_load = tok_rows * devices * route_count // experts
    new_bias = expert_bias + bias_rate * jnp.sign((mean_load - expert_load).astype(F32))
    return (combined.astype(BF16), expert_load, new_bias)


def solution(mesh):
    finer = Mesh(mesh.devices.reshape(mesh.shape["gx"], mesh.shape["gy"], 4, 2), AXES)
    return jax.shard_map(
        layer,
        mesh=finer,
        in_specs=(
            P(AXES, None),
            P(AXES, None),
            P(AXES, None),
            P(AXES, None),
            P(("gx", "gy"), None, GZ),
            P(("gx", "gy"), None, GZ),
            P(("gx", "gy"), GZ, None),
            P(),
        ),
        out_specs=(P(AXES, None), P(), P()),
        check_vma=False,
    )
```

```python
import functools

import jax
import jax.numpy as jnp
from jax import lax
from jax.experimental import pallas as pl
from jax.experimental.pallas import tpu as pltpu
from jax.sharding import Mesh
from jax.sharding import PartitionSpec as P

AXES = ("gx", "gy", "gz_0", "gz_1")
GZ = ("gz_0", "gz_1")
X, Y, Z = "gz_0", "gx", "gy"
EARLY = (X, Y, Z)
LATE = ((X, Y, Z), (Y, Z, X), (Z, X, Y))
INFO = 128
CUTS = (0, 2432, 4864, 7168)
COL_CUTS = (0, 2432, 4864, 7168)
BF16 = jnp.bfloat16
F32 = jnp.float32

bias_rate = 0.001


def exchange(value, axis):
    masks = (1, 3)
    pairs = [(2 * i + c, 2 * (i ^ masks[c]) + c) for i in range(4) for c in range(2)]
    return lax.ppermute(value, (axis, "gz_1"), pairs)


def direct(value, hops):
    masks = (3, 1)
    pairs = []
    for a in range(4):
        for b in range(4):
            for x in range(4):
                for c in range(2):
                    m = masks[c]
                    far = (
                        a ^ (m if Y in hops else 0),
                        b ^ (m if Z in hops else 0),
                        x ^ (m if X in hops else 0),
                    )
                    here = ((a * 4 + b) * 4 + x) * 2 + c
                    pairs.append((here, ((far[0] * 4 + far[1]) * 4 + far[2]) * 2 + c))
    return lax.ppermute(value, AXES, pairs)


def hops_of(n):
    return [axis for k, axis in enumerate(EARLY) if n >> k & 1]


def partner(value):
    return lax.ppermute(value, "gz_1", [(0, 1), (1, 0)])


def canonical(colour, place):
    bits = {LATE[colour][k]: place >> k & 1 for k in range(3)}
    return sum(bits[LATE[0][k]] << k for k in range(3))


VMEM = pl.BlockSpec(memory_space=pltpu.VMEM)
SMEM = pl.BlockSpec(memory_space=pltpu.SMEM)


def rows_kernel(experts, tokens, ids_in, weights_in, out, ids, weights, sem):
    width = tokens.shape[1]
    copies = (
        pltpu.make_async_copy(ids_in, ids, sem.at[0]),
        pltpu.make_async_copy(weights_in, weights, sem.at[1]),
        pltpu.make_async_copy(tokens, out.at[:, pl.ds(0, width)], sem.at[2]),
    )
    for c in copies:
        c.start()
    copies[0].wait()
    copies[1].wait()
    lane = lax.broadcasted_iota(jnp.int32, (tokens.shape[0], INFO), 1)
    info = jnp.zeros((tokens.shape[0], INFO), F32)
    for k in range(ids.shape[1]):
        chosen = ids[:, k : k + 1]
        info += jnp.where(lane == chosen, weights[:, k : k + 1].astype(F32), 0.0)
        info += jnp.where(lane == chosen + experts, 1.0, 0.0)
    out[:, width:] = info.astype(BF16)
    copies[2].wait()


def rows_of(tokens, ids, weights, experts):
    rows, width = tokens.shape
    return pl.pallas_call(
        functools.partial(rows_kernel, experts),
        out_shape=jax.ShapeDtypeStruct((rows, width + INFO), BF16),
        in_specs=[pl.BlockSpec(memory_space=pltpu.HBM)] * 3,
        out_specs=VMEM,
        scratch_shapes=[
            pltpu.VMEM(ids.shape, ids.dtype),
            pltpu.VMEM(weights.shape, weights.dtype),
            pltpu.SemaphoreType.DMA((3,)),
        ],
        compiler_params=pltpu.CompilerParams(vmem_limit_bytes=4 << 20),
        name="token_rows",
    )(tokens, ids, weights)


def near_kernel(x0, x1, x2, w0, w1, w2, w3, acc):
    for i, x in enumerate((x0, x1, x2)):
        width = CUTS[i + 1] - CUTS[i]
        places = [canonical(i, q) for q in range(4)]
        for j, w in enumerate((w0, w1, w2, w3)):
            part = jnp.dot(
                x[:, :width], w[CUTS[i] : CUTS[i + 1], :], preferred_element_type=F32
            )
            for q, s in enumerate(places):
                rows = part[64 * q : 64 * q + 64]
                if i == 0:
                    acc[j, 64 * s : 64 * s + 64, :] = rows
                else:
                    acc[j, 64 * s : 64 * s + 64, :] += rows
            if i == 0:
                for s in range(8):
                    if s not in places:
                        acc[j, 64 * s : 64 * s + 64, :] = jnp.zeros((64, 256), F32)


def far_part_kernel(colour, x, w0, w1, w2, w3, out):
    rows = slice(CUTS[colour], CUTS[colour + 1])
    width = CUTS[colour + 1] - CUTS[colour]
    for j, w in enumerate((w0, w1, w2, w3)):
        out[j] = jnp.dot(x[:, :width], w[rows, :], preferred_element_type=F32)


def hidden_kernel(expert, part0, part1, part2, near_x2, x2, acc, hidden, marks):
    parts = (part0, part1, part2)
    far_places = [{canonical(i, q + 4): 64 * q for q in range(4)} for i in range(3)]

    def total(j, s):
        rows = acc[j, 64 * s : 64 * s + 64, :]
        for i in range(3):
            if s in far_places[i]:
                at = far_places[i][s]
                rows += parts[i][j, at : at + 64, :]
        return rows

    lane = lax.broadcasted_iota(jnp.int32, (64, INFO), 1)
    sums = jnp.zeros((8, INFO), F32)
    for place in range(8):
        s = canonical(2, place)
        source = near_x2 if place < 4 else x2
        at = 64 * (place % 4)
        info = source[at : at + 64, CUTS[3] - CUTS[2] :].astype(F32)
        sums += jnp.sum(info.reshape(8, 8, INFO), axis=0)
        scale = jnp.sum(jnp.where(lane == expert[0], info, 0.0), axis=1, keepdims=True)
        for part in range(2):
            g, u = total(part, s), total(part + 2, s)
            h = g / (1.0 + jnp.exp(-g)) * u * scale
            hidden[64 * s : 64 * s + 64, 256 * part : 256 * part + 256] = h.astype(BF16)
    marks[...] = jnp.sum(sums, axis=0, keepdims=True).astype(jnp.int32)


def load_kernel(*refs):
    count = (len(refs) - 1) // 2
    sem = refs[-1]
    copies = [
        pltpu.make_async_copy(refs[k], refs[count + k], sem.at[k]) for k in range(count)
    ]
    for c in copies:
        c.start()
    for c in copies:
        c.wait()


def in_vmem(*arrays):
    return pl.pallas_call(
        load_kernel,
        out_shape=tuple(jax.ShapeDtypeStruct(a.shape, a.dtype) for a in arrays),
        in_specs=[pl.BlockSpec(memory_space=pl.ANY)] * len(arrays),
        out_specs=(VMEM,) * len(arrays),
        scratch_shapes=[pltpu.SemaphoreType.DMA((len(arrays),))],
        compiler_params=pltpu.CompilerParams(vmem_limit_bytes=4 << 20),
        cost_estimate=pl.CostEstimate(flops=8 << 30, transcendentals=0, bytes_accessed=0),
        name="weights_in",
    )(*arrays)


def cost(parts):
    return pl.CostEstimate(
        flops=2 * 256 * 2389 * 1024 * parts, transcendentals=0, bytes_accessed=0
    )


def gate_up_near(pieces, weights):
    return pl.pallas_call(
        near_kernel,
        out_shape=jax.ShapeDtypeStruct((4, 512, 256), F32),
        in_specs=[VMEM] * 7,
        out_specs=VMEM,
        cost_estimate=cost(3),
        compiler_params=pltpu.CompilerParams(vmem_limit_bytes=8 << 20),
        name="gate_up_near",
    )(*pieces, *weights)


def gate_up_far_part(colour, piece, weights):
    return pl.pallas_call(
        functools.partial(far_part_kernel, colour),
        out_shape=jax.ShapeDtypeStruct((4, 256, 256), F32),
        in_specs=[VMEM] * 5,
        out_specs=VMEM,
        cost_estimate=cost(1),
        compiler_params=pltpu.CompilerParams(vmem_limit_bytes=6 << 20),
    )(piece, *weights)


def hidden_of(expert, parts, near_x2, far_x2, acc):
    return pl.pallas_call(
        hidden_kernel,
        out_shape=(
            jax.ShapeDtypeStruct((512, 512), BF16),
            jax.ShapeDtypeStruct((1, INFO), jnp.int32),
        ),
        in_specs=[SMEM] + [VMEM] * 6,
        out_specs=(VMEM, VMEM),
        cost_estimate=cost(1),
        compiler_params=pltpu.CompilerParams(vmem_limit_bytes=6 << 20),
        name="hidden",
    )(expert, *parts, near_x2, far_x2, acc)


def down_kernel(colour, far, hidden, own, other, out):
    cols = slice(COL_CUTS[colour], COL_CUTS[colour + 1])
    blocks = [canonical(colour, q + (4 if far else 0)) for q in range(4)]
    lhs = jnp.concatenate([hidden[64 * s : 64 * s + 64, :] for s in blocks], axis=0)
    total = jnp.dot(lhs[:, :256], own[:, cols], preferred_element_type=F32)
    total += jnp.dot(lhs[:, 256:], other[:, cols], preferred_element_type=F32)
    out[...] = total.astype(out.dtype)


def down_part(colour, far, hidden, own, other):
    width = COL_CUTS[colour + 1] - COL_CUTS[colour]
    return pl.pallas_call(
        functools.partial(down_kernel, colour, far),
        out_shape=jax.ShapeDtypeStruct((256, width), BF16 if far else F32),
        in_specs=[VMEM] * 3,
        out_specs=VMEM,
        cost_estimate=pl.CostEstimate(
            flops=2 * 256 * 512 * width, transcendentals=0, bytes_accessed=0
        ),
        compiler_params=pltpu.CompilerParams(vmem_limit_bytes=6 << 20),
    )(hidden, own, other)


def layer(
    tokens, expert_ids, slot_ids, route_weight, gate_weight, up_weight, down_weight, expert_bias
):
    experts = lax.axis_size("gx") * lax.axis_size("gy")
    devices = experts * lax.axis_size(GZ)
    tok_rows, width = tokens.shape
    route_count = expert_ids.shape[1]
    own_expert = lax.axis_index("gx") * lax.axis_size("gy") + lax.axis_index("gy")

    gate_own, up_own, down_own = gate_weight[0], up_weight[0], down_weight[0]
    gate_far = partner(gate_own)
    up_far = partner(up_own)
    down_far = partner(down_own)
    gate_own, up_own, down_own = in_vmem(gate_own, up_own, down_own)
    gate_far, up_far = in_vmem(gate_far, up_far)
    (down_far,) = in_vmem(down_far)
    gate_ups = (gate_own, gate_far, up_own, up_far)

    rows = rows_of(tokens, expert_ids, route_weight, experts)
    blocks = [rows]
    for n in range(1, 8):
        blocks.append(direct(rows, hops_of(n)))
    rows = jnp.concatenate(blocks, axis=0)
    ends = (*CUTS[:3], width + INFO)
    pieces = [rows[:, ends[i] : ends[i + 1]] for i in range(3)]
    for step in range(3):
        far_pieces = []
        for i, p in enumerate(pieces):
            far_pieces.append(exchange(p, LATE[i][step]))
        if step < 2:
            pieces = [jnp.concatenate(pair, axis=0) for pair in zip(pieces, far_pieces)]

    acc = gate_up_near(pieces, gate_ups)
    expert = jnp.full((1,), own_expert, jnp.int32)
    parts = [gate_up_far_part(i, far_pieces[i], gate_ups) for i in range(3)]
    hidden, marks = hidden_of(expert, parts, pieces[2], far_pieces[2], acc)

    sent = [down_part(i, True, hidden, down_own, down_far) for i in range(3)]
    kept = []
    for i in range(3):
        kept.append(down_part(i, False, hidden, down_own, down_far))
    for step in (2, 1, 0):
        got = []
        for i in range(3):
            got.append(exchange(sent[i], LATE[i][step]))
        totals = [kept[i] + got[i].astype(F32) for i in range(3)]
        half = totals[0].shape[0] // 2
        if step:
            sent = [t[half:].astype(BF16) for t in totals]
            kept = [t[:half] for t in totals]
    total = jnp.concatenate(totals, axis=1)
    combined = total[:tok_rows]
    for n in range(1, 8):
        block = total[n * tok_rows : (n + 1) * tok_rows].astype(BF16)
        block = direct(block, hops_of(n))
        combined = combined + block.astype(F32)

    other_marks = partner(marks)
    expert_load = (marks + other_marks)[0, experts : 2 * experts]
    mean_load = tok_rows * devices * route_count // experts
    new_bias = expert_bias + bias_rate * jnp.sign((mean_load - expert_load).astype(F32))
    return (combined.astype(BF16), expert_load, new_bias)


def solution(mesh):
    finer = Mesh(mesh.devices.reshape(mesh.shape["gx"], mesh.shape["gy"], 4, 2), AXES)
    return jax.shard_map(
        layer,
        mesh=finer,
        in_specs=(
            P(AXES, None),
            P(AXES, None),
            P(AXES, None),
            P(AXES, None),
            P(("gx", "gy"), None, GZ),
            P(("gx", "gy"), None, GZ),
            P(("gx", "gy"), GZ, None),
            P(),
        ),
        out_specs=(P(AXES, None), P(), P()),
        check_vma=False,
    )
```

```python
import functools

import jax
import jax.numpy as jnp
from jax import lax
from jax.experimental import pallas as pl
from jax.experimental.pallas import tpu as pltpu
from jax.sharding import Mesh
from jax.sharding import PartitionSpec as P

AXES = ("gx", "gy", "gz_0", "gz_1")
GZ = ("gz_0", "gz_1")
X, Y, Z = "gz_0", "gx", "gy"
EARLY = (X, Y, Z)
LATE = ((X, Y, Z), (Y, Z, X), (Z, X, Y))
INFO = 128
CUTS = (0, 2560, 4992, 7168)
COL_CUTS = (0, 2176, 4608, 7168)
BF16 = jnp.bfloat16
F32 = jnp.float32

bias_rate = 0.001


def exchange(value, axis):
    masks = (3, 1)
    pairs = [(2 * i + c, 2 * (i ^ masks[c]) + c) for i in range(4) for c in range(2)]
    return lax.ppermute(value, (axis, "gz_1"), pairs)


def direct(value, hops):
    masks = (1, 3)
    pairs = []
    for a in range(4):
        for b in range(4):
            for x in range(4):
                for c in range(2):
                    m = masks[c]
                    far = (
                        a ^ (m if Y in hops else 0),
                        b ^ (m if Z in hops else 0),
                        x ^ (m if X in hops else 0),
                    )
                    here = ((a * 4 + b) * 4 + x) * 2 + c
                    pairs.append((here, ((far[0] * 4 + far[1]) * 4 + far[2]) * 2 + c))
    return lax.ppermute(value, AXES, pairs)


def hops_of(n):
    return [axis for k, axis in enumerate(EARLY) if n >> k & 1]


def partner(value):
    return lax.ppermute(value, "gz_1", [(0, 1), (1, 0)])


def canonical(colour, place):
    bits = {LATE[colour][k]: place >> k & 1 for k in range(3)}
    return sum(bits[LATE[0][k]] << k for k in range(3))


VMEM = pl.BlockSpec(memory_space=pltpu.VMEM)
SMEM = pl.BlockSpec(memory_space=pltpu.SMEM)


def rows_kernel(experts, tokens, ids_in, weights_in, out, ids, weights, sem):
    width = tokens.shape[1]
    copies = (
        pltpu.make_async_copy(ids_in, ids, sem.at[0]),
        pltpu.make_async_copy(weights_in, weights, sem.at[1]),
        pltpu.make_async_copy(tokens, out.at[:, pl.ds(0, width)], sem.at[2]),
    )
    for c in copies:
        c.start()
    copies[0].wait()
    copies[1].wait()
    lane = lax.broadcasted_iota(jnp.int32, (tokens.shape[0], INFO), 1)
    info = jnp.zeros((tokens.shape[0], INFO), F32)
    for k in range(ids.shape[1]):
        chosen = ids[:, k : k + 1]
        info += jnp.where(lane == chosen, weights[:, k : k + 1].astype(F32), 0.0)
        info += jnp.where(lane == chosen + experts, 1.0, 0.0)
    out[:, width:] = info.astype(BF16)
    copies[2].wait()


def rows_of(tokens, ids, weights, experts):
    rows, width = tokens.shape
    return pl.pallas_call(
        functools.partial(rows_kernel, experts),
        out_shape=jax.ShapeDtypeStruct((rows, width + INFO), BF16),
        in_specs=[pl.BlockSpec(memory_space=pltpu.HBM)] * 3,
        out_specs=VMEM,
        scratch_shapes=[
            pltpu.VMEM(ids.shape, ids.dtype),
            pltpu.VMEM(weights.shape, weights.dtype),
            pltpu.SemaphoreType.DMA((3,)),
        ],
        compiler_params=pltpu.CompilerParams(vmem_limit_bytes=4 << 20),
        name="token_rows",
    )(tokens, ids, weights)


def near_kernel(x0, x1, x2, w0, w1, w2, w3, acc):
    for i, x in enumerate((x0, x1, x2)):
        width = CUTS[i + 1] - CUTS[i]
        places = [canonical(i, q) for q in range(4)]
        for j, w in enumerate((w0, w1, w2, w3)):
            part = jnp.dot(
                x[:, :width], w[CUTS[i] : CUTS[i + 1], :], preferred_element_type=F32
            )
            for q, s in enumerate(places):
                rows = part[64 * q : 64 * q + 64]
                if i == 0:
                    acc[j, 64 * s : 64 * s + 64, :] = rows
                else:
                    acc[j, 64 * s : 64 * s + 64, :] += rows
            if i == 0:
                for s in range(8):
                    if s not in places:
                        acc[j, 64 * s : 64 * s + 64, :] = jnp.zeros((64, 256), F32)


def far_part_kernel(colour, x, w0, w1, w2, w3, out):
    rows = slice(CUTS[colour], CUTS[colour + 1])
    width = CUTS[colour + 1] - CUTS[colour]
    for j, w in enumerate((w0, w1, w2, w3)):
        out[j] = jnp.dot(x[:, :width], w[rows, :], preferred_element_type=F32)


def hidden_kernel(expert, part0, part1, part2, near_x2, x2, acc, hidden, marks):
    parts = (part0, part1, part2)
    far_places = [{canonical(i, q + 4): 64 * q for q in range(4)} for i in range(3)]

    def total(j, s):
        rows = acc[j, 64 * s : 64 * s + 64, :]
        for i in range(3):
            if s in far_places[i]:
                at = far_places[i][s]
                rows += parts[i][j, at : at + 64, :]
        return rows

    lane = lax.broadcasted_iota(jnp.int32, (64, INFO), 1)
    sums = jnp.zeros((8, INFO), F32)
    for place in range(8):
        s = canonical(2, place)
        source = near_x2 if place < 4 else x2
        at = 64 * (place % 4)
        info = source[at : at + 64, CUTS[3] - CUTS[2] :].astype(F32)
        sums += jnp.sum(info.reshape(8, 8, INFO), axis=0)
        scale = jnp.sum(jnp.where(lane == expert[0], info, 0.0), axis=1, keepdims=True)
        for part in range(2):
            g, u = total(part, s), total(part + 2, s)
            h = g / (1.0 + jnp.exp(-g)) * u * scale
            hidden[64 * s : 64 * s + 64, 256 * part : 256 * part + 256] = h.astype(BF16)
    marks[...] = jnp.sum(sums, axis=0, keepdims=True).astype(jnp.int32)


def load_kernel(*refs):
    count = (len(refs) - 1) // 2
    sem = refs[-1]
    copies = [
        pltpu.make_async_copy(refs[k], refs[count + k], sem.at[k]) for k in range(count)
    ]
    for c in copies:
        c.start()
    for c in copies:
        c.wait()


def in_vmem(*arrays):
    return pl.pallas_call(
        load_kernel,
        out_shape=tuple(jax.ShapeDtypeStruct(a.shape, a.dtype) for a in arrays),
        in_specs=[pl.BlockSpec(memory_space=pl.ANY)] * len(arrays),
        out_specs=(VMEM,) * len(arrays),
        scratch_shapes=[pltpu.SemaphoreType.DMA((len(arrays),))],
        compiler_params=pltpu.CompilerParams(vmem_limit_bytes=4 << 20),
        cost_estimate=pl.CostEstimate(flops=8 << 30, transcendentals=0, bytes_accessed=0),
        name="weights_in",
    )(*arrays)


def cost(parts):
    return pl.CostEstimate(
        flops=2 * 256 * 2389 * 1024 * parts, transcendentals=0, bytes_accessed=0
    )


def gate_up_near(pieces, weights):
    return pl.pallas_call(
        near_kernel,
        out_shape=jax.ShapeDtypeStruct((4, 512, 256), F32),
        in_specs=[VMEM] * 7,
        out_specs=VMEM,
        cost_estimate=cost(3),
        compiler_params=pltpu.CompilerParams(vmem_limit_bytes=8 << 20),
        name="gate_up_near",
    )(*pieces, *weights)


def gate_up_far_part(colour, piece, weights):
    return pl.pallas_call(
        functools.partial(far_part_kernel, colour),
        out_shape=jax.ShapeDtypeStruct((4, 256, 256), F32),
        in_specs=[VMEM] * 5,
        out_specs=VMEM,
        cost_estimate=cost(1),
        compiler_params=pltpu.CompilerParams(vmem_limit_bytes=6 << 20),
    )(piece, *weights)


def hidden_of(expert, parts, near_x2, far_x2, acc):
    return pl.pallas_call(
        hidden_kernel,
        out_shape=(
            jax.ShapeDtypeStruct((512, 512), BF16),
            jax.ShapeDtypeStruct((1, INFO), jnp.int32),
        ),
        in_specs=[SMEM] + [VMEM] * 6,
        out_specs=(VMEM, VMEM),
        cost_estimate=cost(1),
        compiler_params=pltpu.CompilerParams(vmem_limit_bytes=6 << 20),
        name="hidden",
    )(expert, *parts, near_x2, far_x2, acc)


def down_kernel(colour, far, hidden, own, other, out):
    cols = slice(COL_CUTS[colour], COL_CUTS[colour + 1])
    blocks = [canonical(colour, q + (4 if far else 0)) for q in range(4)]
    lhs = jnp.concatenate([hidden[64 * s : 64 * s + 64, :] for s in blocks], axis=0)
    total = jnp.dot(lhs[:, :256], own[:, cols], preferred_element_type=F32)
    total += jnp.dot(lhs[:, 256:], other[:, cols], preferred_element_type=F32)
    out[...] = total.astype(out.dtype)


def down_part(colour, far, hidden, own, other):
    width = COL_CUTS[colour + 1] - COL_CUTS[colour]
    return pl.pallas_call(
        functools.partial(down_kernel, colour, far),
        out_shape=jax.ShapeDtypeStruct((256, width), BF16 if far else F32),
        in_specs=[VMEM] * 3,
        out_specs=VMEM,
        cost_estimate=pl.CostEstimate(
            flops=2 * 256 * 512 * width, transcendentals=0, bytes_accessed=0
        ),
        compiler_params=pltpu.CompilerParams(vmem_limit_bytes=6 << 20),
    )(hidden, own, other)


def layer(
    tokens, expert_ids, slot_ids, route_weight, gate_weight, up_weight, down_weight, expert_bias
):
    experts = lax.axis_size("gx") * lax.axis_size("gy")
    devices = experts * lax.axis_size(GZ)
    tok_rows, width = tokens.shape
    route_count = expert_ids.shape[1]
    own_expert = lax.axis_index("gx") * lax.axis_size("gy") + lax.axis_index("gy")

    gate_own, up_own, down_own = gate_weight[0], up_weight[0], down_weight[0]
    gate_far = partner(gate_own)
    up_far = partner(up_own)
    down_far = partner(down_own)
    gate_own, up_own, down_own = in_vmem(gate_own, up_own, down_own)
    gate_far, up_far = in_vmem(gate_far, up_far)
    (down_far,) = in_vmem(down_far)
    gate_ups = (gate_own, gate_far, up_own, up_far)

    rows = rows_of(tokens, expert_ids, route_weight, experts)
    blocks = [rows]
    for n in range(1, 8):
        blocks.append(direct(rows, hops_of(n)))
    rows = jnp.concatenate(blocks, axis=0)
    ends = (*CUTS[:3], width + INFO)
    pieces = [rows[:, ends[i] : ends[i + 1]] for i in range(3)]
    for step in range(3):
        far_pieces = []
        for i, p in enumerate(pieces):
            far_pieces.append(exchange(p, LATE[i][step]))
        if step < 2:
            joined = []
            for i in range(3):
                joined.append(jnp.concatenate([pieces[i], far_pieces[i]], axis=0))
            pieces = joined

    acc = gate_up_near(pieces, gate_ups)
    expert = jnp.full((1,), own_expert, jnp.int32)
    parts = []
    for i in range(3):
        parts.append(gate_up_far_part(i, far_pieces[i], gate_ups))
    hidden, marks = hidden_of(expert, parts, pieces[2], far_pieces[2], acc)

    sent = []
    for i in range(3):
        sent.append(down_part(i, True, hidden, down_own, down_far))
    kept = []
    for i in range(3):
        kept.append(down_part(i, False, hidden, down_own, down_far))
    for step in (2, 1, 0):
        got = []
        for i in range(3):
            got.append(exchange(sent[i], LATE[i][step]))
        totals = []
        for i in range(3):
            totals.append(kept[i] + got[i].astype(F32))
        half = totals[0].shape[0] // 2
        if step:
            sent = [t[half:].astype(BF16) for t in totals]
            kept = [t[:half] for t in totals]
    total = jnp.concatenate(totals, axis=1)
    combined = total[:tok_rows]
    for n in range(1, 8):
        block = total[n * tok_rows : (n + 1) * tok_rows].astype(BF16)
        block = direct(block, hops_of(n))
        combined = combined + block.astype(F32)

    other_marks = partner(marks)
    expert_load = (marks + other_marks)[0, experts : 2 * experts]
    mean_load = tok_rows * devices * route_count // experts
    new_bias = expert_bias + bias_rate * jnp.sign((mean_load - expert_load).astype(F32))
    return (combined.astype(BF16), expert_load, new_bias)


def solution(mesh):
    finer = Mesh(mesh.devices.reshape(mesh.shape["gx"], mesh.shape["gy"], 4, 2), AXES)
    return jax.shard_map(
        layer,
        mesh=finer,
        in_specs=(
            P(AXES, None),
            P(AXES, None),
            P(AXES, None),
            P(AXES, None),
            P(("gx", "gy"), None, GZ),
            P(("gx", "gy"), None, GZ),
            P(("gx", "gy"), GZ, None),
            P(),
        ),
        out_specs=(P(AXES, None), P(), P()),
        check_vma=False,
    )
```

```python
import functools

import jax
import jax.numpy as jnp
from jax import lax
from jax.experimental import pallas as pl
from jax.experimental.pallas import tpu as pltpu
from jax.sharding import Mesh
from jax.sharding import PartitionSpec as P

AXES = ("gx", "gy", "gz_0", "gz_1")
GZ = ("gz_0", "gz_1")
X, Y, Z = "gz_0", "gx", "gy"
EARLY = (X, Y, Z)
LATE = ((X, Y, Z), (Y, Z, X), (Z, X, Y))
INFO = 128
CUTS = (0, 2432, 4864, 7168)
COL_CUTS = (0, 2432, 4864, 7168)
BF16 = jnp.bfloat16
F32 = jnp.float32

bias_rate = 0.001


def exchange(value, axis):
    masks = (3, 1)
    pairs = [(2 * i + c, 2 * (i ^ masks[c]) + c) for i in range(4) for c in range(2)]
    return lax.ppermute(value, (axis, "gz_1"), pairs)


def direct(value, hops):
    masks = (1, 3)
    pairs = []
    for a in range(4):
        for b in range(4):
            for x in range(4):
                for c in range(2):
                    m = masks[c]
                    far = (
                        a ^ (m if Y in hops else 0),
                        b ^ (m if Z in hops else 0),
                        x ^ (m if X in hops else 0),
                    )
                    here = ((a * 4 + b) * 4 + x) * 2 + c
                    pairs.append((here, ((far[0] * 4 + far[1]) * 4 + far[2]) * 2 + c))
    return lax.ppermute(value, AXES, pairs)


def hops_of(n):
    return [axis for k, axis in enumerate(EARLY) if n >> k & 1]


def partner(value):
    return lax.ppermute(value, "gz_1", [(0, 1), (1, 0)])


def canonical(colour, place):
    bits = {LATE[colour][k]: place >> k & 1 for k in range(3)}
    return sum(bits[LATE[0][k]] << k for k in range(3))


VMEM = pl.BlockSpec(memory_space=pltpu.VMEM)
SMEM = pl.BlockSpec(memory_space=pltpu.SMEM)


def rows_kernel(experts, tokens, routes, out):
    width = tokens.shape[1]
    count = routes.shape[1] // 2
    out[:, :width] = tokens[...]
    lane = lax.broadcasted_iota(jnp.int32, (tokens.shape[0], INFO), 1).astype(F32)
    info = jnp.zeros((tokens.shape[0], INFO), F32)
    for k in range(count):
        chosen = routes[:, k : k + 1]
        info += jnp.where(lane == chosen, routes[:, count + k : count + k + 1], 0.0)
        info += jnp.where(lane == chosen + experts, 1.0, 0.0)
    out[:, width:] = info.astype(BF16)


def rows_of(tokens, ids, weights, experts):
    rows, width = tokens.shape
    routes = jnp.concatenate([ids.astype(F32), weights.astype(F32)], axis=1)
    return pl.pallas_call(
        functools.partial(rows_kernel, experts),
        out_shape=jax.ShapeDtypeStruct((rows, width + INFO), BF16),
        in_specs=[VMEM] * 2,
        out_specs=VMEM,
        compiler_params=pltpu.CompilerParams(vmem_limit_bytes=4 << 20),
        name="token_rows",
    )(tokens, routes)


def near_kernel(x0, x1, x2, w0, w1, w2, w3, acc):
    for i, x in enumerate((x0, x1, x2)):
        width = CUTS[i + 1] - CUTS[i]
        places = [canonical(i, q) for q in range(4)]
        for j, w in enumerate((w0, w1, w2, w3)):
            part = jnp.dot(
                x[:, :width], w[CUTS[i] : CUTS[i + 1], :], preferred_element_type=F32
            )
            for q, s in enumerate(places):
                rows = part[64 * q : 64 * q + 64]
                if i == 0:
                    acc[j, 64 * s : 64 * s + 64, :] = rows
                else:
                    acc[j, 64 * s : 64 * s + 64, :] += rows
            if i == 0:
                for s in range(8):
                    if s not in places:
                        acc[j, 64 * s : 64 * s + 64, :] = jnp.zeros((64, 256), F32)


def far_part_kernel(colour, x, w0, w1, w2, w3, out):
    rows = slice(CUTS[colour], CUTS[colour + 1])
    width = CUTS[colour + 1] - CUTS[colour]
    for j, w in enumerate((w0, w1, w2, w3)):
        out[j] = jnp.dot(x[:, :width], w[rows, :], preferred_element_type=F32)


def hidden_kernel(expert, part0, part1, part2, near_x2, x2, acc, hidden, marks):
    parts = (part0, part1, part2)
    far_places = [{canonical(i, q + 4): 64 * q for q in range(4)} for i in range(3)]

    def total(j, s):
        rows = acc[j, 64 * s : 64 * s + 64, :]
        for i in range(3):
            if s in far_places[i]:
                at = far_places[i][s]
                rows += parts[i][j, at : at + 64, :]
        return rows

    lane = lax.broadcasted_iota(jnp.int32, (64, INFO), 1)
    sums = jnp.zeros((8, INFO), F32)
    for place in range(8):
        s = canonical(2, place)
        source = near_x2 if place < 4 else x2
        at = 64 * (place % 4)
        info = source[at : at + 64, CUTS[3] - CUTS[2] :].astype(F32)
        sums += jnp.sum(info.reshape(8, 8, INFO), axis=0)
        scale = jnp.sum(jnp.where(lane == expert[0], info, 0.0), axis=1, keepdims=True)
        for part in range(2):
            g, u = total(part, s), total(part + 2, s)
            h = g / (1.0 + jnp.exp(-g)) * u * scale
            hidden[64 * s : 64 * s + 64, 256 * part : 256 * part + 256] = h.astype(BF16)
    marks[...] = jnp.sum(sums, axis=0, keepdims=True).astype(jnp.int32)


def load_kernel(*refs):
    count = (len(refs) - 1) // 2
    sem = refs[-1]
    copies = [
        pltpu.make_async_copy(refs[k], refs[count + k], sem.at[k]) for k in range(count)
    ]
    for c in copies:
        c.start()
    for c in copies:
        c.wait()


def in_vmem(*arrays):
    return pl.pallas_call(
        load_kernel,
        out_shape=tuple(jax.ShapeDtypeStruct(a.shape, a.dtype) for a in arrays),
        in_specs=[pl.BlockSpec(memory_space=pl.ANY)] * len(arrays),
        out_specs=(VMEM,) * len(arrays),
        scratch_shapes=[pltpu.SemaphoreType.DMA((len(arrays),))],
        compiler_params=pltpu.CompilerParams(vmem_limit_bytes=4 << 20),
        cost_estimate=pl.CostEstimate(flops=8 << 30, transcendentals=0, bytes_accessed=0),
        name="weights_in",
    )(*arrays)


def cost(parts):
    return pl.CostEstimate(
        flops=2 * 256 * 2389 * 1024 * parts, transcendentals=0, bytes_accessed=0
    )


def gate_up_near(pieces, weights):
    return pl.pallas_call(
        near_kernel,
        out_shape=jax.ShapeDtypeStruct((4, 512, 256), F32),
        in_specs=[VMEM] * 7,
        out_specs=VMEM,
        cost_estimate=cost(3),
        compiler_params=pltpu.CompilerParams(vmem_limit_bytes=8 << 20),
        name="gate_up_near",
    )(*pieces, *weights)


def gate_up_far_part(colour, piece, weights):
    return pl.pallas_call(
        functools.partial(far_part_kernel, colour),
        out_shape=jax.ShapeDtypeStruct((4, 256, 256), F32),
        in_specs=[VMEM] * 5,
        out_specs=VMEM,
        cost_estimate=cost(1),
        compiler_params=pltpu.CompilerParams(vmem_limit_bytes=6 << 20),
    )(piece, *weights)


def hidden_of(expert, parts, near_x2, far_x2, acc):
    return pl.pallas_call(
        hidden_kernel,
        out_shape=(
            jax.ShapeDtypeStruct((512, 512), BF16),
            jax.ShapeDtypeStruct((1, INFO), jnp.int32),
        ),
        in_specs=[SMEM] + [VMEM] * 6,
        out_specs=(VMEM, VMEM),
        cost_estimate=cost(1),
        compiler_params=pltpu.CompilerParams(vmem_limit_bytes=6 << 20),
        name="hidden",
    )(expert, *parts, near_x2, far_x2, acc)


def down_kernel(colour, far, hidden, own, other, out):
    cols = slice(COL_CUTS[colour], COL_CUTS[colour + 1])
    blocks = [canonical(colour, q + (4 if far else 0)) for q in range(4)]
    lhs = jnp.concatenate([hidden[64 * s : 64 * s + 64, :] for s in blocks], axis=0)
    total = jnp.dot(lhs[:, :256], own[:, cols], preferred_element_type=F32)
    total += jnp.dot(lhs[:, 256:], other[:, cols], preferred_element_type=F32)
    out[...] = total.astype(out.dtype)


def down_part(colour, far, hidden, own, other):
    width = COL_CUTS[colour + 1] - COL_CUTS[colour]
    return pl.pallas_call(
        functools.partial(down_kernel, colour, far),
        out_shape=jax.ShapeDtypeStruct((256, width), BF16 if far else F32),
        in_specs=[VMEM] * 3,
        out_specs=VMEM,
        cost_estimate=pl.CostEstimate(
            flops=2 * 256 * 512 * width, transcendentals=0, bytes_accessed=0
        ),
        compiler_params=pltpu.CompilerParams(vmem_limit_bytes=6 << 20),
    )(hidden, own, other)


def layer(
    tokens, expert_ids, slot_ids, route_weight, gate_weight, up_weight, down_weight, expert_bias
):
    experts = lax.axis_size("gx") * lax.axis_size("gy")
    devices = experts * lax.axis_size(GZ)
    tok_rows, width = tokens.shape
    route_count = expert_ids.shape[1]
    own_expert = lax.axis_index("gx") * lax.axis_size("gy") + lax.axis_index("gy")

    gate_own, up_own, down_own = gate_weight[0], up_weight[0], down_weight[0]
    gate_far = partner(gate_own)
    up_far = partner(up_own)
    down_far = partner(down_own)
    gate_own, up_own, down_own = in_vmem(gate_own, up_own, down_own)
    gate_far, up_far = in_vmem(gate_far, up_far)
    (down_far,) = in_vmem(down_far)
    gate_ups = (gate_own, gate_far, up_own, up_far)

    rows = rows_of(tokens, expert_ids, route_weight, experts)
    blocks = [rows]
    for n in range(1, 8):
        blocks.append(direct(rows, hops_of(n)))
    rows = jnp.concatenate(blocks, axis=0)
    ends = (*CUTS[:3], width + INFO)
    pieces = [rows[:, ends[i] : ends[i + 1]] for i in range(3)]
    for step in range(3):
        far_pieces = []
        for i, p in enumerate(pieces):
            far_pieces.append(exchange(p, LATE[i][step]))
        if step < 2:
            joined = []
            for i in range(3):
                joined.append(jnp.concatenate([pieces[i], far_pieces[i]], axis=0))
            pieces = joined

    acc = gate_up_near(pieces, gate_ups)
    expert = jnp.full((1,), own_expert, jnp.int32)
    parts = []
    for i in range(3):
        parts.append(gate_up_far_part(i, far_pieces[i], gate_ups))
    hidden, marks = hidden_of(expert, parts, pieces[2], far_pieces[2], acc)

    sent = []
    for i in range(3):
        sent.append(down_part(i, True, hidden, down_own, down_far))
    kept = []
    for i in range(3):
        kept.append(down_part(i, False, hidden, down_own, down_far))
    for step in (2, 1, 0):
        got = []
        for i in range(3):
            got.append(exchange(sent[i], LATE[i][step]))
        totals = []
        for i in range(3):
            totals.append(kept[i] + got[i].astype(F32))
        half = totals[0].shape[0] // 2
        if step:
            sent = [t[half:].astype(BF16) for t in totals]
            kept = [t[:half] for t in totals]
    total = jnp.concatenate(totals, axis=1)
    combined = total[:tok_rows]
    for n in range(1, 8):
        block = total[n * tok_rows : (n + 1) * tok_rows].astype(BF16)
        block = direct(block, hops_of(n))
        combined = combined + block.astype(F32)

    other_marks = partner(marks)
    expert_load = (marks + other_marks)[0, experts : 2 * experts]
    mean_load = tok_rows * devices * route_count // experts
    new_bias = expert_bias + bias_rate * jnp.sign((mean_load - expert_load).astype(F32))
    return (combined.astype(BF16), expert_load, new_bias)


def solution(mesh):
    finer = Mesh(mesh.devices.reshape(mesh.shape["gx"], mesh.shape["gy"], 4, 2), AXES)
    return jax.shard_map(
        layer,
        mesh=finer,
        in_specs=(
            P(AXES, None),
            P(AXES, None),
            P(AXES, None),
            P(AXES, None),
            P(("gx", "gy"), None, GZ),
            P(("gx", "gy"), None, GZ),
            P(("gx", "gy"), GZ, None),
            P(),
        ),
        out_specs=(P(AXES, None), P(), P()),
        check_vma=False,
    )
```

```python
import functools

import jax
import jax.numpy as jnp
from jax import lax
from jax.experimental import pallas as pl
from jax.experimental.pallas import tpu as pltpu
from jax.sharding import Mesh
from jax.sharding import PartitionSpec as P

AXES = ("gx", "gy", "gz_0", "gz_1")
GZ = ("gz_0", "gz_1")
X, Y, Z = "gz_0", "gx", "gy"
LATE = ((X, Y, Z), (Y, Z, X), (Z, X, Y))
INFO = 128
CUTS = (0, 2432, 4864, 7168)
COL_CUTS = (0, 2304, 4736, 7168)
BF16 = jnp.bfloat16
F32 = jnp.float32

bias_rate = 0.001


def exchange(value, axis):
    masks = (3, 1)
    pairs = [(2 * i + c, 2 * (i ^ masks[c]) + c) for i in range(4) for c in range(2)]
    return lax.ppermute(value, (axis, "gz_1"), pairs)


def cubes():
    index, groups, seen = lambda a, b, x, c: ((a * 4 + b) * 4 + x) * 2 + c, [], set()
    for a in range(4):
        for b in range(4):
            for x in range(4):
                for c, m in enumerate((1, 3)):
                    if index(a, b, x, c) not in seen:
                        group = [
                            index(a ^ (m * (n >> 2 & 1)), b ^ (m * (n >> 1 & 1)), x ^ (m * (n & 1)), c)
                            for n in range(8)
                        ]
                        groups.append(group)
                        seen.update(group)
    return groups


def swap(blocks):
    return lax.all_to_all(blocks, AXES, 0, 0, axis_index_groups=cubes(), tiled=True)


def partner(value):
    return lax.ppermute(value, "gz_1", [(0, 1), (1, 0)])


def canonical(colour, place):
    bits = {LATE[colour][k]: place >> k & 1 for k in range(3)}
    return sum(bits[LATE[0][k]] << k for k in range(3))


VMEM = pl.BlockSpec(memory_space=pltpu.VMEM)
SMEM = pl.BlockSpec(memory_space=pltpu.SMEM)


def rows_kernel(experts, tokens, routes, out):
    width = tokens.shape[1]
    count = routes.shape[1] // 2
    out[:, :width] = tokens[...]
    lane = lax.broadcasted_iota(jnp.int32, (tokens.shape[0], INFO), 1).astype(F32)
    info = jnp.zeros((tokens.shape[0], INFO), F32)
    for k in range(count):
        chosen = routes[:, k : k + 1]
        info += jnp.where(lane == chosen, routes[:, count + k : count + k + 1], 0.0)
        info += jnp.where(lane == chosen + experts, 1.0, 0.0)
    out[:, width:] = info.astype(BF16)


def rows_of(tokens, ids, weights, experts):
    rows, width = tokens.shape
    routes = jnp.concatenate([ids.astype(F32), weights.astype(F32)], axis=1)
    return pl.pallas_call(
        functools.partial(rows_kernel, experts),
        out_shape=jax.ShapeDtypeStruct((rows, width + INFO), BF16),
        in_specs=[VMEM] * 2,
        out_specs=VMEM,
        compiler_params=pltpu.CompilerParams(vmem_limit_bytes=4 << 20),
        name="token_rows",
    )(tokens, routes)


def near_kernel(x0, x1, x2, w0, w1, w2, w3, acc):
    for i, x in enumerate((x0, x1, x2)):
        width = CUTS[i + 1] - CUTS[i]
        places = [canonical(i, q) for q in range(4)]
        for j, w in enumerate((w0, w1, w2, w3)):
            part = jnp.dot(
                x[:, :width], w[CUTS[i] : CUTS[i + 1], :], preferred_element_type=F32
            )
            for q, s in enumerate(places):
                rows = part[64 * q : 64 * q + 64]
                if i == 0:
                    acc[j, 64 * s : 64 * s + 64, :] = rows
                else:
                    acc[j, 64 * s : 64 * s + 64, :] += rows
            if i == 0:
                for s in range(8):
                    if s not in places:
                        acc[j, 64 * s : 64 * s + 64, :] = jnp.zeros((64, 256), F32)


def far_part_kernel(colour, x, w0, w1, w2, w3, out):
    rows = slice(CUTS[colour], CUTS[colour + 1])
    width = CUTS[colour + 1] - CUTS[colour]
    for j, w in enumerate((w0, w1, w2, w3)):
        out[j] = jnp.dot(x[:, :width], w[rows, :], preferred_element_type=F32)


def hidden_kernel(expert, part0, part1, part2, near_x2, x2, acc, hidden, marks):
    parts = (part0, part1, part2)
    far_places = [{canonical(i, q + 4): 64 * q for q in range(4)} for i in range(3)]

    def total(j, s):
        rows = acc[j, 64 * s : 64 * s + 64, :]
        for i in range(3):
            if s in far_places[i]:
                at = far_places[i][s]
                rows += parts[i][j, at : at + 64, :]
        return rows

    lane = lax.broadcasted_iota(jnp.int32, (64, INFO), 1)
    sums = jnp.zeros((8, INFO), F32)
    for place in range(8):
        s = canonical(2, place)
        source = near_x2 if place < 4 else x2
        at = 64 * (place % 4)
        info = source[at : at + 64, CUTS[3] - CUTS[2] :].astype(F32)
        sums += jnp.sum(info.reshape(8, 8, INFO), axis=0)
        scale = jnp.sum(jnp.where(lane == expert[0], info, 0.0), axis=1, keepdims=True)
        for part in range(2):
            g, u = total(part, s), total(part + 2, s)
            h = g / (1.0 + jnp.exp(-g)) * u * scale
            hidden[64 * s : 64 * s + 64, 256 * part : 256 * part + 256] = h.astype(BF16)
    marks[...] = jnp.sum(sums, axis=0, keepdims=True).astype(jnp.int32)


def load_kernel(*refs):
    count = (len(refs) - 1) // 2
    sem = refs[-1]
    copies = [
        pltpu.make_async_copy(refs[k], refs[count + k], sem.at[k]) for k in range(count)
    ]
    for c in copies:
        c.start()
    for c in copies:
        c.wait()


def in_vmem(*arrays):
    return pl.pallas_call(
        load_kernel,
        out_shape=tuple(jax.ShapeDtypeStruct(a.shape, a.dtype) for a in arrays),
        in_specs=[pl.BlockSpec(memory_space=pl.ANY)] * len(arrays),
        out_specs=(VMEM,) * len(arrays),
        scratch_shapes=[pltpu.SemaphoreType.DMA((len(arrays),))],
        compiler_params=pltpu.CompilerParams(vmem_limit_bytes=4 << 20),
        cost_estimate=pl.CostEstimate(flops=8 << 30, transcendentals=0, bytes_accessed=0),
        name="weights_in",
    )(*arrays)


def cost(parts):
    return pl.CostEstimate(
        flops=2 * 256 * 2389 * 1024 * parts, transcendentals=0, bytes_accessed=0
    )


def gate_up_near(pieces, weights):
    return pl.pallas_call(
        near_kernel,
        out_shape=jax.ShapeDtypeStruct((4, 512, 256), F32),
        in_specs=[VMEM] * 7,
        out_specs=VMEM,
        cost_estimate=cost(3),
        compiler_params=pltpu.CompilerParams(vmem_limit_bytes=8 << 20),
        name="gate_up_near",
    )(*pieces, *weights)


def gate_up_far_part(colour, piece, weights):
    return pl.pallas_call(
        functools.partial(far_part_kernel, colour),
        out_shape=jax.ShapeDtypeStruct((4, 256, 256), F32),
        in_specs=[VMEM] * 5,
        out_specs=VMEM,
        cost_estimate=cost(1),
        compiler_params=pltpu.CompilerParams(vmem_limit_bytes=6 << 20),
    )(piece, *weights)


def hidden_of(expert, parts, near_x2, far_x2, acc):
    return pl.pallas_call(
        hidden_kernel,
        out_shape=(
            jax.ShapeDtypeStruct((512, 512), BF16),
            jax.ShapeDtypeStruct((1, INFO), jnp.int32),
        ),
        in_specs=[SMEM] + [VMEM] * 6,
        out_specs=(VMEM, VMEM),
        cost_estimate=cost(1),
        compiler_params=pltpu.CompilerParams(vmem_limit_bytes=6 << 20),
        name="hidden",
    )(expert, *parts, near_x2, far_x2, acc)


def down_kernel(colour, far, hidden, own, other, out):
    cols = slice(COL_CUTS[colour], COL_CUTS[colour + 1])
    blocks = [canonical(colour, q + (4 if far else 0)) for q in range(4)]
    lhs = jnp.concatenate([hidden[64 * s : 64 * s + 64, :] for s in blocks], axis=0)
    total = jnp.dot(lhs[:, :256], own[:, cols], preferred_element_type=F32)
    total += jnp.dot(lhs[:, 256:], other[:, cols], preferred_element_type=F32)
    out[...] = total.astype(out.dtype)


def down_part(colour, far, hidden, own, other):
    width = COL_CUTS[colour + 1] - COL_CUTS[colour]
    return pl.pallas_call(
        functools.partial(down_kernel, colour, far),
        out_shape=jax.ShapeDtypeStruct((256, width), BF16 if far else F32),
        in_specs=[VMEM] * 3,
        out_specs=VMEM,
        cost_estimate=pl.CostEstimate(
            flops=2 * 256 * 512 * width, transcendentals=0, bytes_accessed=0
        ),
        compiler_params=pltpu.CompilerParams(vmem_limit_bytes=6 << 20),
    )(hidden, own, other)


def layer(
    tokens, expert_ids, slot_ids, route_weight, gate_weight, up_weight, down_weight, expert_bias
):
    experts = lax.axis_size("gx") * lax.axis_size("gy")
    devices = experts * lax.axis_size(GZ)
    tok_rows, width = tokens.shape
    route_count = expert_ids.shape[1]
    own_expert = lax.axis_index("gx") * lax.axis_size("gy") + lax.axis_index("gy")

    gate_own, up_own, down_own = gate_weight[0], up_weight[0], down_weight[0]
    gate_far = partner(gate_own)
    up_far = partner(up_own)
    down_far = partner(down_own)
    gate_own, up_own, down_own = in_vmem(gate_own, up_own, down_own)
    gate_far, up_far = in_vmem(gate_far, up_far)
    (down_far,) = in_vmem(down_far)
    gate_ups = (gate_own, gate_far, up_own, up_far)

    rows = rows_of(tokens, expert_ids, route_weight, experts)
    rows = swap(jnp.broadcast_to(rows[None], (8, *rows.shape))).reshape(64, width + INFO)
    ends = (*CUTS[:3], width + INFO)
    pieces = [rows[:, ends[i] : ends[i + 1]] for i in range(3)]
    for step in range(3):
        far_pieces = []
        for i, p in enumerate(pieces):
            far_pieces.append(exchange(p, LATE[i][step]))
        if step < 2:
            joined = []
            for i in range(3):
                joined.append(jnp.concatenate([pieces[i], far_pieces[i]], axis=0))
            pieces = joined

    acc = gate_up_near(pieces, gate_ups)
    expert = jnp.full((1,), own_expert, jnp.int32)
    parts = []
    for i in range(3):
        parts.append(gate_up_far_part(i, far_pieces[i], gate_ups))
    hidden, marks = hidden_of(expert, parts, pieces[2], far_pieces[2], acc)

    sent = []
    for i in range(3):
        sent.append(down_part(i, True, hidden, down_own, down_far))
    kept = []
    for i in range(3):
        kept.append(down_part(i, False, hidden, down_own, down_far))
    for step in (2, 1, 0):
        got = []
        for i in range(3):
            got.append(exchange(sent[i], LATE[i][step]))
        totals = []
        for i in range(3):
            totals.append(kept[i] + got[i].astype(F32))
        half = totals[0].shape[0] // 2
        if step:
            sent = [t[half:].astype(BF16) for t in totals]
            kept = [t[:half] for t in totals]
    total = jnp.concatenate(totals, axis=1)
    blocks = swap(total.astype(BF16).reshape(8, tok_rows, width))
    combined = jnp.sum(blocks.astype(F32), axis=0)

    other_marks = partner(marks)
    expert_load = (marks + other_marks)[0, experts : 2 * experts]
    mean_load = tok_rows * devices * route_count // experts
    new_bias = expert_bias + bias_rate * jnp.sign((mean_load - expert_load).astype(F32))
    return (combined.astype(BF16), expert_load, new_bias)


def solution(mesh):
    finer = Mesh(mesh.devices.reshape(mesh.shape["gx"], mesh.shape["gy"], 4, 2), AXES)
    return jax.shard_map(
        layer,
        mesh=finer,
        in_specs=(
            P(AXES, None),
            P(AXES, None),
            P(AXES, None),
            P(AXES, None),
            P(("gx", "gy"), None, GZ),
            P(("gx", "gy"), None, GZ),
            P(("gx", "gy"), GZ, None),
            P(),
        ),
        out_specs=(P(AXES, None), P(), P()),
        check_vma=False,
    )
```
